256 devices in a mesh: rep: 4 (over y), shard: 64 (over x, z, core).
Axes of the slice: x: 4, y: 4, z: 8, core: 2. Of those that a mesh axis runs over, the one named last changes fastest.
Arguments:
- item_ids: int32 [512, 1024], P(('rep', 'shard')), may hold values from 0 to 524287, as said below
- seq_lengths: int32 [4, 128], P('rep'), may hold values from 64 to 1024, as said below
- seq_owner: int32 [4, 128], P('rep'), may hold values from 0 to 63, as said below
- row_home: int32 [524288], replicated, may hold values from 0 to 524287, as said below
- item_table: bfloat16 [524288, 256], P('shard', 'rep'), may hold values from -6 to 6
- proj_weight: bfloat16 [256, 1024], replicated, may hold values from -0.375 to 0.375
- out_weight: bfloat16 [256, 256], replicated, may hold values from -0.375 to 0.375
Outputs:
- mixed: bfloat16 [512, 1024, 256], P(('rep', 'shard'))
The draws below stay inside these ranges and needn't reach their ends.
Inputs may be any that keep to these rules, and one draw needn't show every extreme that they name: `item_ids`: for every history and every shard index k, at most 32 of its 1024 slots name items with row_home[item] // 8192 == k; in every draw one shard index is named by exactly 32 slots of every history. `row_home`: A permutation of the table rows. `seq_lengths`: each group has a history of exactly 1024 live events. `seq_owner`: every shard index owns exactly 2 histories of each group.
All inputs are finite; a program needn't handle non-finite values.
Results may differ from the reference program's by a relative error of at most 0.0058.
Values may be sent and summed in bfloat16 or wider, within the bound.
A program may use at most 64 MiB of HBM per device.

```python
import math
import jax
import jax.numpy as jnp
from jax import lax

D = 256
HEADS = 4
SEQ_LEN = 1024
SEQ_DEV = 2
ROWS_DEV = 8192
CAP_SEQ = 32
SEQS_GRP = 128
USERS = 512
ITEMS = 524288
N_REP = 4


def sequence_plan(key):
    owners_count = SEQS_GRP // SEQ_DEV
    index = jnp.arange(SEQS_GRP, dtype=jnp.int32)
    lengths = jax.random.randint(jax.random.fold_in(key, 11), (N_REP, SEQS_GRP), SEQ_LEN // 16, SEQ_LEN + 1, dtype=jnp.int32)
    longest = jax.random.randint(jax.random.fold_in(key, 12), (N_REP, 1), 0, SEQS_GRP, dtype=jnp.int32)
    lengths = jnp.where(index[None, :] == longest, SEQ_LEN, lengths)
    score = lengths * SEQS_GRP + index[None, :]
    ranked = jnp.argsort(-score, axis=1).astype(jnp.int32)
    rank = jnp.argsort(ranked, axis=1).astype(jnp.int32)
    sweep = rank // owners_count
    within = rank % owners_count
    owners = jnp.where(sweep % 2 == 0, within, owners_count - 1 - within)
    return (lengths.astype(jnp.int32), owners.astype(jnp.int32))


def table_plan(key):
    return jax.random.permutation(jax.random.fold_in(key, 21), ITEMS).astype(jnp.int32)


def draw_seq_lengths(key, part):
    return sequence_plan(key)[0]


def draw_seq_owner(key, part):
    return sequence_plan(key)[1]


def draw_row_home(key, part):
    return table_plan(key)


def draw_item_ids(key, part):
    places = table_plan(key)
    inverse = jnp.zeros((ITEMS,), jnp.int32).at[places].set(jnp.arange(ITEMS, dtype=jnp.int32))
    shards = ITEMS // ROWS_DEV
    pool = jnp.repeat(jnp.arange(shards, dtype=jnp.int32), CAP_SEQ, total_repeat_length=shards * CAP_SEQ)
    hottest = jax.random.randint(jax.random.fold_in(key, 22), (), 0, shards, dtype=jnp.int32)
    noise = jax.random.randint(jax.random.fold_in(key, 23), (USERS, shards * CAP_SEQ), 0, 2 ** 30, dtype=jnp.int32)
    score = jnp.where(pool[None, :] == hottest, 0, 1 + noise)
    picked = jnp.argsort(score, axis=1, stable=True)[:, :SEQ_LEN].astype(jnp.int32)
    owner = pool[picked]
    mixing = jax.random.randint(jax.random.fold_in(key, 24), (USERS, SEQ_LEN), 0, 2 ** 30, dtype=jnp.int32)
    shuffle = jnp.argsort(mixing, axis=1, stable=True).astype(jnp.int32)
    owner = jnp.take_along_axis(owner, shuffle, axis=1)
    local = jax.random.randint(jax.random.fold_in(key, 25), (USERS, SEQ_LEN), 0, ROWS_DEV, dtype=jnp.int32)
    return inverse[owner * ROWS_DEV + local]


def levels(own_key, shape, cuts, low, top_value):
    def one(position, shards_of):
        heights = jax.random.uniform(jax.random.fold_in(jax.random.fold_in(own_key, 6), position), (shards_of,), jnp.float32, low / len(cuts), top_value / len(cuts))
        return jnp.repeat(jnp.exp(heights), shape[position] // shards_of).reshape((-1,) + (1,) * (len(shape) - position - 1))

    factor_of = one(*cuts[0])
    for cut in cuts[1:]:
        factor_of = factor_of * one(*cut)
    return factor_of


def gaussian(rng, extent, deviation, reach, split=(), kind=jnp.bfloat16):
    array = deviation * jax.random.normal(rng, extent, jnp.float32)
    if split:
        array = array * levels(rng, extent, split, -0.22, 0.18)
    return jnp.clip(array, -reach, reach).astype(kind)


def setup_inputs(seed: int = 0) -> dict:
    streams_of = jax.random.split(jax.random.key(seed), 8)
    return {
        "item_ids": draw_item_ids(jax.random.fold_in(streams_of[7], 71), 0),
        "seq_lengths": draw_seq_lengths(jax.random.fold_in(streams_of[7], 71), 0),
        "seq_owner": draw_seq_owner(jax.random.fold_in(streams_of[7], 71), 0),
        "row_home": draw_row_home(jax.random.fold_in(streams_of[7], 71), 0),
        "item_table": gaussian(streams_of[4], (ITEMS, D), 1.0, 6.0, ((0, 64), (1, 4))),
        "proj_weight": gaussian(streams_of[5], (D, 4 * D), D ** -0.5, 0.375),
        "out_weight": gaussian(streams_of[6], (D, D), D ** -0.5, 0.375),
    }


EPSILON = 1e-06

def layer_norm(values):
    center = values - lax.optimization_barrier(jnp.mean(values, axis=-1, keepdims=True))
    spread = lax.optimization_barrier(jnp.mean(center * center, axis=-1, keepdims=True))
    return center * lax.rsqrt(spread + EPSILON)

def sequence_layer(embedded, length, proj_weight, out_weight):
    seq_len, width = embedded.shape
    head_dim = width // HEADS
    normed = layer_norm(embedded.astype(jnp.float32)).astype(jnp.bfloat16)
    proj = jax.nn.silu(jnp.dot(normed, proj_weight, preferred_element_type=jnp.float32)).astype(jnp.bfloat16)
    gate = proj[:, :width].astype(jnp.float32)
    values = proj[:, width:2 * width].reshape(seq_len, HEADS, head_dim).astype(jnp.float32)
    queries = proj[:, 2 * width:3 * width].reshape(seq_len, HEADS, head_dim).astype(jnp.float32)
    keys = proj[:, 3 * width:].reshape(seq_len, HEADS, head_dim).astype(jnp.float32)
    scores = jnp.einsum('qhd,khd->hqk', queries, keys, precision=lax.Precision.HIGHEST) * (1.0 / math.sqrt(head_dim))
    places = jnp.arange(seq_len, dtype=jnp.int32)
    keep = places[None, :] <= places[:, None]
    weights = jnp.where(keep[None], jax.nn.silu(scores) / length.astype(jnp.float32), 0.0).astype(jnp.bfloat16)
    attended = jnp.einsum('hqk,khd->qhd', weights.astype(jnp.float32), values, precision=lax.Precision.HIGHEST).reshape(seq_len, width)
    gated = (layer_norm(attended) * gate).astype(jnp.bfloat16)
    mixed = embedded.astype(jnp.float32) + jnp.dot(gated, out_weight, preferred_element_type=jnp.float32)
    live = (places < length)[:, None]
    return jnp.where(live, mixed, 0.0).astype(jnp.bfloat16)

def reference(item_ids, seq_lengths, seq_owner, row_home, item_table, proj_weight, out_weight):
    order = jnp.argsort(seq_owner, axis=1, stable=True).astype(jnp.int32)
    offsets = jnp.arange(N_REP, dtype=jnp.int32)[:, None] * SEQS_GRP
    chosen = (order + offsets).reshape(-1).astype(jnp.int32)
    lengths = jnp.take_along_axis(seq_lengths, order, axis=1).reshape(-1)

    def run(pair):
        index, length = pair
        ids = item_ids[index]
        rows = jnp.take(item_table, row_home[ids], axis=0)
        return sequence_layer(rows, length, proj_weight, out_weight)
    return lax.map(run, (chosen, lengths))
```

```python
import math

import jax
import jax.numpy as jnp
from jax import lax
from jax.experimental import pallas as pl
from jax.experimental.pallas import tpu as pltpu
from jax.sharding import PartitionSpec as P

HEADS = 4
EPSILON = 1e-06
BLOCK = 256
CAP = 32
F32 = jnp.float32
BF16 = jnp.bfloat16
I32 = jnp.int32


def column_of(row, size):
    pieces = []
    step = 128
    eye = lax.broadcasted_iota(I32, (step, step), 0) == lax.broadcasted_iota(I32, (step, step), 1)
    for i in range(size // step):
        part = row[:, i * step : (i + 1) * step].astype(F32)
        pieces.append(jnp.sum(jnp.where(eye, part, 0.0), axis=1, keepdims=True))
    return jnp.concatenate(pieces, axis=0)


def contract_rows(left, right):
    return lax.dot_general(left, right, (((0,), (0,)), ((), ())), preferred_element_type=F32)


def plan_kernel(ids_smem, len_smem, ids_ref, home_ref, out_ref, stage):
    seq_len = ids_ref.shape[1]
    shards = out_ref.shape[0]
    rows_dev = home_ref.shape[0] * 128 // shards
    step = 32

    for seq in range(2):

        def fetch(c, carry):
            for i in range(step):
                t = c * step + i
                row = ids_smem[seq, t] // 128
                stage[pl.ds(seq * seq_len + t, 1), :] = home_ref[pl.ds(row, 1), :]
            return carry

        lax.fori_loop(0, seq_len // step, fetch, 0)

    place = lax.broadcasted_iota(I32, (seq_len, 1), 0)
    lane = lax.broadcasted_iota(I32, (seq_len, 128), 1)
    lane_k = lax.broadcasted_iota(I32, (seq_len, shards), 1)
    below = (
        lax.broadcasted_iota(I32, (128, 128), 1) < lax.broadcasted_iota(I32, (128, 128), 0)
    ).astype(BF16)
    own = ((place // 16) == lane_k).astype(BF16)
    result = jnp.zeros((shards, 128), F32)
    for seq in range(2):
        ids = column_of(ids_ref[seq : seq + 1, :], seq_len).astype(I32)
        picked = jnp.where(
            (ids & 127) == lane, stage[pl.ds(seq * seq_len, seq_len), :].astype(F32), 0.0
        )
        home = jnp.sum(picked, axis=1, keepdims=True).astype(I32)
        target = home // rows_dev
        row = home & (rows_dev - 1)
        live = place < len_smem[seq]
        onehot = jnp.where((target == lane_k) & live, 1.0, 0.0)
        onehot16 = onehot.astype(BF16)
        carry = jnp.zeros((1, shards), F32)
        ranks = []
        for b in range(seq_len // 128):
            part = onehot[b * 128 : (b + 1) * 128]
            before = jnp.dot(below, part.astype(BF16), preferred_element_type=F32) + carry
            ranks.append(jnp.sum(before * part, axis=1, keepdims=True))
            carry = carry + jnp.sum(part, axis=0, keepdims=True)
        rank = jnp.concatenate(ranks, axis=0).astype(I32)
        at_rank = lane == rank + seq * CAP
        count = jnp.where(lane == 96 + seq, 1.0, 0.0)
        high = jnp.where(at_rank, (row & ~127).astype(F32), count)
        low = jnp.where(at_rank, (row & 127).astype(F32), 0.0)
        result = result + contract_rows(onehot16, high.astype(BF16))
        result = result + contract_rows(onehot16, low.astype(BF16))
        slot = jnp.where(live, target * CAP + rank, 0)
        at_place = lane == (place & 15) + (64 + seq * 16)
        high = jnp.where(at_place, (slot & ~127).astype(F32), 0.0)
        low = jnp.where(at_place, (slot & 127).astype(F32), 0.0)
        result = result + contract_rows(own, high.astype(BF16))
        result = result + contract_rows(own, low.astype(BF16))
    out_ref[...] = result.astype(I32)


def plan_requests(item_ids, lengths, row_home, shards):
    seq_dev, seq_len = item_ids.shape
    return pl.pallas_call(
        plan_kernel,
        out_shape=jax.ShapeDtypeStruct((shards, 128), I32),
        in_specs=[
            pl.BlockSpec(memory_space=pltpu.SMEM),
            pl.BlockSpec(memory_space=pltpu.SMEM),
            pl.BlockSpec(memory_space=pltpu.VMEM),
            pl.BlockSpec(memory_space=pltpu.VMEM),
        ],
        out_specs=pl.BlockSpec(memory_space=pltpu.VMEM),
        scratch_shapes=[pltpu.VMEM((seq_dev * seq_len, 128), I32)],
        name="plan",
    )(item_ids, lengths, item_ids, row_home.reshape(-1, 128))


def gather_kernel(order_ref, asked_ref, table_ref, out_ref, rows, stage):
    step = pl.program_id(0)
    width, rows_dev = table_ref.shape
    owners = out_ref.shape[0]
    chunk = 256

    @pl.when(step == 0)
    def _():
        eye = (
            lax.broadcasted_iota(I32, (chunk, chunk), 0)
            == lax.broadcasted_iota(I32, (chunk, chunk), 1)
        ).astype(BF16)

        def turn(c, carry):
            at = pl.multiple_of(c * chunk, chunk)
            rows[pl.ds(at, chunk), :] = lax.dot_general(
                eye, table_ref[:, pl.ds(at, chunk)], (((1,), (1,)), ((), ())), preferred_element_type=F32
            )
            return carry

        lax.fori_loop(0, rows_dev // chunk, turn, 0)

    unroll = 8

    def history(q, carry):
        hist = order_ref[step * owners * 2 + q]
        source = hist // 2
        half = hist & 1
        count = asked_ref[source, 96 + half]

        def fetch(c, carry):
            for i in range(unroll):
                j = c * unroll + i
                row = asked_ref[source, half * CAP + j]
                stage[pl.ds(q * CAP + j, 1), :] = rows[pl.ds(row, 1), :]
            return carry

        return lax.fori_loop(0, (count + unroll - 1) // unroll, fetch, carry)

    lax.fori_loop(0, owners * 2, history, 0)
    out_ref[...] = stage[...].astype(BF16).reshape(out_ref.shape)


def gather_rows(order, asked, table, shards):
    width, rows_dev = table.shape
    owners = 8
    return pl.pallas_call(
        gather_kernel,
        grid=(shards // owners,),
        out_shape=jax.ShapeDtypeStruct((shards, 2 * CAP, width), BF16),
        in_specs=[
            pl.BlockSpec(memory_space=pltpu.SMEM),
            pl.BlockSpec(memory_space=pltpu.SMEM),
            pl.BlockSpec((width, rows_dev), lambda i: (0, 0)),
        ],
        out_specs=pl.BlockSpec((owners, 2 * CAP, width), lambda i: (i, 0, 0)),
        scratch_shapes=[
            pltpu.VMEM((rows_dev, width), F32),
            pltpu.VMEM((owners * 2 * CAP, width), F32),
        ],
        compiler_params=pltpu.CompilerParams(vmem_limit_bytes=48 * 1024 * 1024),
        name="gather",
    )(order, asked, table)


def normed_rows(values):
    center = values - jnp.mean(values, axis=-1, keepdims=True)
    spread = jnp.mean(center * center, axis=-1, keepdims=True)
    return center * lax.rsqrt(spread + EPSILON)


def gated_linear(half):
    return half + half * jnp.tanh(half)


def layer_kernel(
    slots_ref, len_ref, got_ref, proj_ref, outw_ref, mixed_ref,
    flat, emb, gates, vals, quer, keys, att,
):
    seq = pl.program_id(0)
    seq_len, width = mixed_ref.shape[1:]
    head = width // HEADS
    length = len_ref[seq]
    flat[...] = got_ref[...].reshape(flat.shape).astype(F32)
    unroll = 16

    def fetch(c, carry):
        for i in range(unroll):
            t = c * unroll + i
            emb[pl.ds(t, 1), :] = flat[pl.ds(slots_ref[seq, t], 1), :]
        return carry

    lax.fori_loop(0, (length + unroll - 1) // unroll, fetch, 0)
    blocks = (length + BLOCK - 1) // BLOCK
    place = lax.broadcasted_iota(I32, (BLOCK, 1), 0)

    def project(b, carry):
        at = pl.multiple_of(b * BLOCK, BLOCK)
        span = pl.ds(at, BLOCK)
        rows = jnp.where(place + at < length, emb[span, :], 0.0)
        emb[span, :] = rows
        normed = normed_rows(rows).astype(BF16)
        for part, ref in enumerate((gates, vals, quer, keys)):
            raw = jnp.dot(
                normed, proj_ref[:, part * width : (part + 1) * width], preferred_element_type=F32
            )
            made = gated_linear(raw * 0.5).astype(BF16)
            if part == 0:
                ref[span, :] = made
            else:
                if part == 2:
                    made = made * (0.5 / math.sqrt(head))
                for h in range(HEADS):
                    ref[h, span, :] = made[:, h * head : (h + 1) * head]
        return carry

    lax.fori_loop(0, blocks, project, 0)
    inverse = 1.0 / length.astype(F32)
    for b in range(seq_len // BLOCK):

        @pl.when(b * BLOCK < length)
        def _(b=b):
            reach = (b + 1) * BLOCK
            keep = lax.broadcasted_iota(I32, (BLOCK, BLOCK), 1) <= lax.broadcasted_iota(
                I32, (BLOCK, BLOCK), 0
            )

            def attend(h, carry):
                query = quer[h, b * BLOCK : reach, :]
                scores = lax.dot_general(
                    query, keys[h, :reach, :], (((1,), (1,)), ((), ())), preferred_element_type=F32
                )
                weights = gated_linear(scores)
                last = jnp.where(keep, weights[:, b * BLOCK :], 0.0).astype(BF16)
                if b:
                    last = jnp.concatenate([weights[:, : b * BLOCK].astype(BF16), last], axis=1)
                att[h] = jnp.dot(last, vals[h, :reach, :], preferred_element_type=F32)
                return carry

            lax.fori_loop(0, HEADS, attend, 0)
            whole = jnp.concatenate([att[h] for h in range(HEADS)], axis=1) * inverse
            gated = (normed_rows(whole) * gates[b * BLOCK : reach, :].astype(F32)).astype(BF16)
            mixed = emb[b * BLOCK : reach, :] + jnp.dot(
                gated, outw_ref[...], preferred_element_type=F32
            )
            live = place + b * BLOCK < length
            mixed_ref[0, b * BLOCK : reach, :] = jnp.where(live, mixed, 0.0).astype(BF16)

        @pl.when(b * BLOCK >= length)
        def _(b=b):
            mixed_ref[0, b * BLOCK : (b + 1) * BLOCK, :] = jnp.zeros((BLOCK, width), BF16)


def layer(slots, lengths, got, proj_weight, out_weight):
    shards, seq_dev, cap, width = got.shape
    seq_len = slots.shape[1]
    head = width // HEADS
    return pl.pallas_call(
        layer_kernel,
        grid=(seq_dev,),
        out_shape=jax.ShapeDtypeStruct((seq_dev, seq_len, width), BF16),
        in_specs=[
            pl.BlockSpec(memory_space=pltpu.SMEM),
            pl.BlockSpec(memory_space=pltpu.SMEM),
            pl.BlockSpec((shards, 1, cap, width), lambda i: (0, i, 0, 0)),
            pl.BlockSpec((width, 4 * width), lambda i: (0, 0)),
            pl.BlockSpec((width, width), lambda i: (0, 0)),
        ],
        out_specs=pl.BlockSpec((1, seq_len, width), lambda i: (i, 0, 0)),
        scratch_shapes=[
            pltpu.VMEM((shards * cap, width), F32),
            pltpu.VMEM((seq_len, width), F32),
            pltpu.VMEM((seq_len, width), BF16),
            pltpu.VMEM((HEADS, seq_len, head), BF16),
            pltpu.VMEM((HEADS, seq_len, head), BF16),
            pltpu.VMEM((HEADS, seq_len, head), BF16),
            pltpu.VMEM((HEADS, BLOCK, head), F32),
        ],
        compiler_params=pltpu.CompilerParams(vmem_limit_bytes=48 * 1024 * 1024),
        name="layer",
    )(slots, lengths, got, proj_weight, out_weight)


def body(item_ids, seq_lengths, seq_owner, row_home, item_table, proj_weight, out_weight):
    shards = lax.axis_size("shard")
    me = lax.axis_index("shard")
    seq_dev, seq_len = item_ids.shape
    width = proj_weight.shape[0]
    owners = seq_owner[0]
    lengths = seq_lengths[0]
    table = lax.all_gather(item_table.T, "rep", axis=0, tiled=True)
    order = jnp.argsort(owners, stable=True)
    my_lengths = lengths[lax.dynamic_slice_in_dim(order, me * seq_dev, seq_dev)]
    held = lax.dynamic_slice_in_dim(lengths, me * seq_dev, seq_dev)
    asked = plan_requests(item_ids, held, row_home, shards)
    asked = lax.all_to_all(
        asked.reshape(shards, 1, 128), "shard", split_axis=0, concat_axis=0, tiled=True
    ).reshape(shards, 128)
    rows = gather_rows(order, asked, table, shards)
    chunk = seq_len // shards
    maps = jnp.take(asked[:, 64 : 64 + 2 * chunk].reshape(2 * shards, chunk), order, axis=0)
    maps = maps.reshape(shards, 1, seq_dev * chunk)
    maps = jnp.concatenate([maps // CAP, maps % CAP], axis=2).astype(BF16)
    maps = jnp.pad(maps, ((0, 0), (0, 7), (0, width - 4 * chunk)))
    got = lax.all_to_all(
        jnp.concatenate([rows, maps], axis=1), "shard", split_axis=0, concat_axis=0, tiled=True
    )
    slots = got[:, 2 * CAP, : 4 * chunk].astype(I32)
    slots = slots[:, : 2 * chunk] * CAP + slots[:, 2 * chunk :]
    slots = slots.reshape(shards, seq_dev, chunk).transpose(1, 0, 2).reshape(seq_dev, seq_len)
    got = got[:, : 2 * CAP].reshape(shards, seq_dev, CAP, width)
    return layer(slots, my_lengths, got, proj_weight, out_weight)


def solution(mesh):
    in_specs = (
        P(("rep", "shard"), None),
        P("rep", None),
        P("rep", None),
        P(),
        P("shard", "rep"),
        P(),
        P(),
    )
    out_specs = P(("rep", "shard"), None, None)
    return jax.shard_map(body, mesh=mesh, in_specs=in_specs, out_specs=out_specs, check_vma=False)
```

```python
import math

import jax
import jax.numpy as jnp
from jax import lax
from jax.experimental import pallas as pl
from jax.experimental.pallas import tpu as pltpu
from jax.sharding import PartitionSpec as P

HEADS = 4
EPSILON = 1e-06
BLOCK = 256
CAP = 32
F32 = jnp.float32
BF16 = jnp.bfloat16
I32 = jnp.int32


def column_of(row, size):
    pieces = []
    step = 128
    eye = lax.broadcasted_iota(I32, (step, step), 0) == lax.broadcasted_iota(I32, (step, step), 1)
    for i in range(size // step):
        part = row[:, i * step : (i + 1) * step].astype(F32)
        pieces.append(jnp.sum(jnp.where(eye, part, 0.0), axis=1, keepdims=True))
    return jnp.concatenate(pieces, axis=0)


def contract_rows(left, right):
    return lax.dot_general(left, right, (((0,), (0,)), ((), ())), preferred_element_type=F32)


def plan_kernel(ids_smem, len_smem, ids_ref, home_ref, out_ref, stage):
    seq_len = ids_ref.shape[1]
    shards = out_ref.shape[0]
    rows_dev = home_ref.shape[0] * 128 // shards
    step = 32

    for seq in range(2):

        def fetch(c, carry):
            for i in range(step):
                t = c * step + i
                row = ids_smem[seq, t] // 128
                stage[pl.ds(seq * seq_len + t, 1), :] = home_ref[pl.ds(row, 1), :]
            return carry

        lax.fori_loop(0, seq_len // step, fetch, 0)

    place = lax.broadcasted_iota(I32, (seq_len, 1), 0)
    lane = lax.broadcasted_iota(I32, (seq_len, 128), 1)
    lane_k = lax.broadcasted_iota(I32, (seq_len, shards), 1)
    below = (
        lax.broadcasted_iota(I32, (128, 128), 1) < lax.broadcasted_iota(I32, (128, 128), 0)
    ).astype(BF16)
    own = ((place // 16) == lane_k).astype(BF16)
    result = jnp.zeros((shards, 128), F32)
    for seq in range(2):
        ids = column_of(ids_ref[seq : seq + 1, :], seq_len).astype(I32)
        picked = jnp.where(
            (ids & 127) == lane, stage[pl.ds(seq * seq_len, seq_len), :].astype(F32), 0.0
        )
        home = jnp.sum(picked, axis=1, keepdims=True).astype(I32)
        target = home // rows_dev
        row = home & (rows_dev - 1)
        live = place < len_smem[seq]
        onehot = jnp.where((target == lane_k) & live, 1.0, 0.0)
        onehot16 = onehot.astype(BF16)
        carry = jnp.zeros((1, shards), F32)
        ranks = []
        for b in range(seq_len // 128):
            part = onehot[b * 128 : (b + 1) * 128]
            before = jnp.dot(below, part.astype(BF16), preferred_element_type=F32) + carry
            ranks.append(jnp.sum(before * part, axis=1, keepdims=True))
            carry = carry + jnp.sum(part, axis=0, keepdims=True)
        rank = jnp.concatenate(ranks, axis=0).astype(I32)
        at_rank = lane == rank + seq * CAP
        count = jnp.where(lane == 96 + seq, 1.0, 0.0)
        high = jnp.where(at_rank, (row & ~127).astype(F32), count)
        low = jnp.where(at_rank, (row & 127).astype(F32), 0.0)
        result = result + contract_rows(onehot16, high.astype(BF16))
        result = result + contract_rows(onehot16, low.astype(BF16))
        slot = jnp.where(live, target * CAP + rank, 0)
        at_place = lane == (place & 15) + (64 + seq * 16)
        high = jnp.where(at_place, (slot & ~127).astype(F32), 0.0)
        low = jnp.where(at_place, (slot & 127).astype(F32), 0.0)
        result = result + contract_rows(own, high.astype(BF16))
        result = result + contract_rows(own, low.astype(BF16))
    out_ref[...] = result.astype(I32)


def plan_requests(item_ids, lengths, row_home, shards):
    seq_dev, seq_len = item_ids.shape
    return pl.pallas_call(
        plan_kernel,
        out_shape=jax.ShapeDtypeStruct((shards, 128), I32),
        in_specs=[
            pl.BlockSpec(memory_space=pltpu.SMEM),
            pl.BlockSpec(memory_space=pltpu.SMEM),
            pl.BlockSpec(memory_space=pltpu.VMEM),
            pl.BlockSpec(memory_space=pltpu.VMEM),
        ],
        out_specs=pl.BlockSpec(memory_space=pltpu.VMEM),
        scratch_shapes=[pltpu.VMEM((seq_dev * seq_len, 128), I32)],
        name="plan",
    )(item_ids, lengths, item_ids, row_home.reshape(-1, 128))


def exchange_kernel(
    order_ref, asked_ref, table_ref,
    own_got, pair_got, far_got, maps_got,
    asked_all, asked_smem, table_in, left_in, right_in, far_in,
    own_rows, pair_rows, far_rows, stage,
    own_out, pair_out, far_out, maps_out,
    local_sem, asked_send, asked_recv, side_send, side_recv, row_send, row_recv,
):
    shards = asked_ref.shape[0]
    reps = 4
    cols, rows_dev = table_ref.shape
    me = lax.axis_index("shard")
    rep = lax.axis_index("rep")
    right = lax.rem(rep + 1, reps)
    left = lax.rem(rep + reps - 1, reps)
    chunk = min(256, rows_dev)

    load = pltpu.make_async_copy(table_ref, table_in, local_sem.at[0])
    load.start()
    barrier = pltpu.get_barrier_semaphore()

    def greet(i, carry):
        peer = lax.rem(me + i, shards)
        pl.semaphore_signal(
            barrier, inc=1, device_id={"shard": peer}, device_id_type=pl.DeviceIdType.MESH
        )
        return carry

    lax.fori_loop(1, shards, greet, 0)
    for side in (left, right):
        pl.semaphore_signal(
            barrier, inc=1, device_id={"rep": side}, device_id_type=pl.DeviceIdType.MESH
        )

    eye = (
        lax.broadcasted_iota(I32, (chunk, chunk), 0) == lax.broadcasted_iota(I32, (chunk, chunk), 1)
    ).astype(BF16)

    def turn(upper, lower, rows):
        def one(c, carry):
            at = pl.multiple_of(c * chunk, chunk)
            both = jnp.concatenate([upper[:, pl.ds(at, chunk)], lower[:, pl.ds(at, chunk)]], axis=0)
            rows[pl.ds(at, chunk), :] = lax.dot_general(
                eye, both, (((1,), (1,)), ((), ())), preferred_element_type=F32
            )
            return carry

        lax.fori_loop(0, rows_dev // chunk, one, 0)

    load.wait()
    pl.semaphore_wait(barrier, shards + 1)

    def side_copy(source, target, slot, side):
        return pltpu.make_async_remote_copy(
            src_ref=source,
            dst_ref=target,
            send_sem=side_send.at[slot],
            recv_sem=side_recv.at[slot],
            device_id={"rep": side},
            device_id_type=pl.DeviceIdType.MESH,
        )

    def shard_copy(source, target, send, recv, peer):
        return pltpu.make_async_remote_copy(
            src_ref=source,
            dst_ref=target,
            send_sem=send,
            recv_sem=recv,
            device_id={"shard": peer},
            device_id_type=pl.DeviceIdType.MESH,
        )

    def ask(i, carry):
        peer = lax.rem(me + i, shards)
        shard_copy(
            asked_ref.at[peer], asked_all.at[me], asked_send, asked_recv, peer
        ).start()
        return carry

    lax.fori_loop(1, shards, ask, 0)
    keep = pltpu.make_async_copy(asked_ref.at[me], asked_all.at[me], local_sem.at[1])
    keep.start()
    to_right = side_copy(table_in, left_in, 0, right)
    to_left = side_copy(table_in, right_in, 1, left)
    to_right.start()
    to_left.start()
    turn(table_in, table_in, own_rows)
    keep.wait()
    others = pl.ds(0, shards - 1)
    shard_copy(asked_ref.at[others], asked_all.at[others], asked_send, asked_recv, me).wait()
    spill = pltpu.make_async_copy(asked_all, asked_smem, local_sem.at[2])
    spill.start()
    spill.wait()

    first_half = lax.broadcasted_iota(I32, (1, 2 * cols), 1) < cols

    def send_to(out, got, kind, peer):
        shard_copy(out.at[peer], got.at[me], row_send.at[kind], row_recv.at[kind], peer).start()

    def finish(out, got, kind):
        local = pltpu.make_async_copy(out.at[me], got.at[me], local_sem.at[3 + kind])
        local.start()
        local.wait()

    def sweep(pick, out, got, kind, paired, extra=None):
        def owner(i, carry):
            peer = lax.rem(me + i + 1, shards)
            sources = []
            offsets = []
            for q in range(2):
                hist = order_ref[2 * peer + q]
                sources.append(hist // 2)
                offsets.append(lax.rem(hist, 2) * CAP)
            if extra is not None:
                for q in range(2):
                    extra[peer, pl.ds(q, 1), :] = asked_all[sources[q]]
            slot = lax.rem(i, 2)
            if paired:
                for j in range(CAP):
                    one = pick[pl.ds(asked_smem[sources[0], 0, offsets[0] + j], 1), :]
                    two = pick[pl.ds(asked_smem[sources[1], 0, offsets[1] + j], 1), :]
                    stage[slot, pl.ds(j, 1), :] = jnp.where(first_half, one, two)
                out[peer] = stage[slot, :CAP, :].astype(BF16)
            else:
                for q in range(2):
                    for j in range(CAP):
                        stage[slot, pl.ds(q * CAP + j, 1), :] = pick[
                            pl.ds(asked_smem[sources[q], 0, offsets[q] + j], 1), :
                        ]
                out[peer] = stage[slot].astype(BF16)

            @pl.when(i > 0)
            def _():
                before = lax.rem(me + i, shards)
                send_to(out, got, kind, before)
                if extra is not None:
                    send_to(extra, maps_got, 3, before)

            return carry

        lax.fori_loop(0, shards, owner, 0)

    sweep(own_rows, own_out, own_got, 0, True, maps_out)
    to_right.wait_recv()
    to_left.wait_recv()
    half = cols // 2
    on_right = side_copy(left_in.at[pl.ds(0, half)], far_in.at[pl.ds(0, half)], 2, right)
    on_left = side_copy(right_in.at[pl.ds(half, half)], far_in.at[pl.ds(half, half)], 3, left)
    on_right.start()
    on_left.start()
    turn(left_in, right_in, pair_rows)
    sweep(pair_rows, pair_out, pair_got, 1, False)
    on_right.wait_recv()
    on_left.wait_recv()
    turn(far_in, far_in, far_rows)
    sweep(far_rows, far_out, far_got, 2, True)
    for kind, (out, got) in enumerate(
        ((own_out, own_got), (pair_out, pair_got), (far_out, far_got), (maps_out, maps_got))
    ):
        finish(out, got, kind)
    for copy in (to_right, to_left, on_right, on_left):
        copy.wait_send()
    for kind, (out, got) in enumerate(
        ((own_out, own_got), (pair_out, pair_got), (far_out, far_got), (maps_out, maps_got))
    ):
        shard_copy(
            out.at[others], got.at[others], row_send.at[kind], row_recv.at[kind], me
        ).wait()


def exchange_rows(order, asked, table):
    shards = asked.shape[0]
    cols, rows_dev = table.shape
    wide = 2 * cols
    any_space = pl.BlockSpec(memory_space=pl.ANY)
    shapes = (
        ((shards, CAP, wide), BF16),
        ((shards, 2 * CAP, wide), BF16),
        ((shards, CAP, wide), BF16),
        ((shards, 2, 128), I32),
    )
    return pl.pallas_call(
        exchange_kernel,
        out_shape=[jax.ShapeDtypeStruct(*shape) for shape in shapes],
        in_specs=[
            pl.BlockSpec(memory_space=pltpu.SMEM),
            pl.BlockSpec(memory_space=pltpu.VMEM),
            any_space,
        ],
        out_specs=[any_space] * 4,
        scratch_shapes=[
            pltpu.VMEM((shards, 1, 128), I32),
            pltpu.SMEM((shards, 1, 128), I32),
            pltpu.VMEM((cols, rows_dev), BF16),
            pltpu.VMEM((cols, rows_dev), BF16),
            pltpu.VMEM((cols, rows_dev), BF16),
            pltpu.VMEM((cols, rows_dev), BF16),
            pltpu.VMEM((rows_dev, wide), F32),
            pltpu.VMEM((rows_dev, wide), F32),
            pltpu.VMEM((rows_dev, wide), F32),
            pltpu.VMEM((2, 2 * CAP, wide), F32),
            *[pltpu.VMEM(*shape) for shape in shapes],
            pltpu.SemaphoreType.DMA((7,)),
            pltpu.SemaphoreType.DMA,
            pltpu.SemaphoreType.DMA,
            pltpu.SemaphoreType.DMA((4,)),
            pltpu.SemaphoreType.DMA((4,)),
            pltpu.SemaphoreType.DMA((4,)),
            pltpu.SemaphoreType.DMA((4,)),
        ],
        compiler_params=pltpu.CompilerParams(
            collective_id=0, has_side_effects=True, vmem_limit_bytes=40 * 1024 * 1024
        ),
        name="exchange",
    )(order, asked.reshape(shards, 1, 128), table)


def normed_rows(values):
    center = values - jnp.mean(values, axis=-1, keepdims=True)
    spread = jnp.mean(center * center, axis=-1, keepdims=True)
    return center * lax.rsqrt(spread + EPSILON)


def gated_linear(half):
    return half + half * jnp.tanh(half)


def layer_kernel(
    maps_ref, info_ref, own_ref, pair_ref, far_ref, proj_ref, outw_ref, mixed_ref,
    flat, emb, gates, vals, quer, keys, att,
):
    seq = pl.program_id(0)
    seq_len, width = mixed_ref.shape[1:]
    head = width // HEADS
    length = info_ref[seq]
    offset = 64 + 16 * info_ref[2 + seq]
    rep = info_ref[4]
    shards, cap = own_ref.shape[:2]
    side = width // 4
    group = 8
    first_half = lax.broadcasted_iota(I32, (1, 2 * side), 1) < side
    swapped = seq == 1

    for r in range(4):

        @pl.when(rep == r)
        def _(r=r):
            def place_blocks(c, carry):
                span = pl.ds(c * group, group)
                rows = group * cap
                parts = {}
                for name, ref in (("own", own_ref), ("far", far_ref)):
                    part = ref[span].reshape(rows, 2 * side).astype(F32)
                    other = pltpu.roll(part, side, 1)
                    parts[name] = (
                        jnp.where(swapped, other, part),
                        jnp.where(swapped, part, other),
                    )
                pair = pair_ref[span].reshape(rows, 2 * side).astype(F32)
                turned = pltpu.roll(pair, side, 1)
                parts["left"] = (pair, turned)
                parts["right"] = (turned, pair)
                names = ("own", "right", "far", "left")
                at = pl.multiple_of(c * rows, rows)
                for tile in range(2):
                    low = parts[names[(2 * tile - r) % 4]][0]
                    high = parts[names[(2 * tile + 1 - r) % 4]][1]
                    flat[pl.ds(at, rows), tile * 2 * side : (tile + 1) * 2 * side] = jnp.where(
                        first_half, low, high
                    )
                return carry

            lax.fori_loop(0, shards // group, place_blocks, 0)

    unroll = 16

    def fetch(c, carry):
        for i in range(unroll):
            t = c * unroll + i
            slot = maps_ref[c, seq, offset + i]
            emb[pl.ds(t, 1), :] = flat[pl.ds(slot, 1), :]
        return carry

    lax.fori_loop(0, (length + unroll - 1) // unroll, fetch, 0)
    blocks = (length + BLOCK - 1) // BLOCK
    place = lax.broadcasted_iota(I32, (BLOCK, 1), 0)

    def project(b, carry):
        at = pl.multiple_of(b * BLOCK, BLOCK)
        span = pl.ds(at, BLOCK)
        rows = jnp.where(place + at < length, emb[span, :], 0.0)
        emb[span, :] = rows
        normed = normed_rows(rows).astype(BF16)
        for part, ref in enumerate((gates, vals, quer, keys)):
            raw = jnp.dot(
                normed, proj_ref[:, part * width : (part + 1) * width], preferred_element_type=F32
            )
            made = gated_linear(raw * 0.5).astype(BF16)
            if part == 0:
                ref[span, :] = made
            else:
                if part == 2:
                    made = made * (0.5 / math.sqrt(head))
                for h in range(HEADS):
                    ref[h, span, :] = made[:, h * head : (h + 1) * head]
        return carry

    lax.fori_loop(0, blocks, project, 0)
    inverse = 1.0 / length.astype(F32)
    for b in range(seq_len // BLOCK):

        @pl.when(b * BLOCK < length)
        def _(b=b):
            reach = (b + 1) * BLOCK
            keep = lax.broadcasted_iota(I32, (BLOCK, BLOCK), 1) <= lax.broadcasted_iota(
                I32, (BLOCK, BLOCK), 0
            )

            def attend(h, carry):
                query = quer[h, b * BLOCK : reach, :]
                scores = lax.dot_general(
                    query, keys[h, :reach, :], (((1,), (1,)), ((), ())), preferred_element_type=F32
                )
                weights = gated_linear(scores)
                last = jnp.where(keep, weights[:, b * BLOCK :], 0.0).astype(BF16)
                if b:
                    last = jnp.concatenate([weights[:, : b * BLOCK].astype(BF16), last], axis=1)
                att[h] = jnp.dot(last, vals[h, :reach, :], preferred_element_type=F32)
                return carry

            lax.fori_loop(0, HEADS, attend, 0)
            whole = jnp.concatenate([att[h] for h in range(HEADS)], axis=1) * inverse
            gated = (normed_rows(whole) * gates[b * BLOCK : reach, :].astype(F32)).astype(BF16)
            mixed = emb[b * BLOCK : reach, :] + jnp.dot(
                gated, outw_ref[...], preferred_element_type=F32
            )
            live = place + b * BLOCK < length
            mixed_ref[0, b * BLOCK : reach, :] = jnp.where(live, mixed, 0.0).astype(BF16)

        @pl.when(b * BLOCK >= length)
        def _(b=b):
            mixed_ref[0, b * BLOCK : (b + 1) * BLOCK, :] = jnp.zeros((BLOCK, width), BF16)


def layer(maps, info, own, pair, far, proj_weight, out_weight, seq_len):
    shards, cap, wide = own.shape
    seq_dev = 2
    width = proj_weight.shape[0]
    head = width // HEADS
    return pl.pallas_call(
        layer_kernel,
        grid=(seq_dev,),
        out_shape=jax.ShapeDtypeStruct((seq_dev, seq_len, width), BF16),
        in_specs=[
            pl.BlockSpec(memory_space=pltpu.SMEM),
            pl.BlockSpec(memory_space=pltpu.SMEM),
            pl.BlockSpec((shards, cap, wide), lambda i: (0, 0, 0)),
            pl.BlockSpec((shards, cap, wide), lambda i: (0, i, 0)),
            pl.BlockSpec((shards, cap, wide), lambda i: (0, 0, 0)),
            pl.BlockSpec((width, 4 * width), lambda i: (0, 0)),
            pl.BlockSpec((width, width), lambda i: (0, 0)),
        ],
        out_specs=pl.BlockSpec((1, seq_len, width), lambda i: (i, 0, 0)),
        scratch_shapes=[
            pltpu.VMEM((shards * cap, width), F32),
            pltpu.VMEM((seq_len, width), F32),
            pltpu.VMEM((seq_len, width), BF16),
            pltpu.VMEM((HEADS, seq_len, head), BF16),
            pltpu.VMEM((HEADS, seq_len, head), BF16),
            pltpu.VMEM((HEADS, seq_len, head), BF16),
            pltpu.VMEM((HEADS, BLOCK, head), F32),
        ],
        compiler_params=pltpu.CompilerParams(vmem_limit_bytes=48 * 1024 * 1024),
        name="layer",
    )(maps, info, own, pair, far, proj_weight, out_weight)


def body(item_ids, seq_lengths, seq_owner, row_home, item_table, proj_weight, out_weight):
    shards = lax.axis_size("shard")
    me = lax.axis_index("shard")
    seq_dev, seq_len = item_ids.shape
    owners = seq_owner[0]
    lengths = seq_lengths[0]
    order = jnp.argsort(owners, stable=True)
    mine = lax.dynamic_slice_in_dim(order, me * seq_dev, seq_dev)
    held = lax.dynamic_slice_in_dim(lengths, me * seq_dev, seq_dev)
    asked = plan_requests(item_ids, held, row_home, shards)
    own, pair, far, maps = exchange_rows(order, asked, item_table.T)
    rep = lax.axis_index("rep").reshape(1)
    info = jnp.concatenate([lengths[mine], mine % 2, rep])
    return layer(maps, info, own, pair, far, proj_weight, out_weight, seq_len)


def solution(mesh):
    in_specs = (
        P(("rep", "shard"), None),
        P("rep", None),
        P("rep", None),
        P(),
        P("shard", "rep"),
        P(),
        P(),
    )
    out_specs = P(("rep", "shard"), None, None)
    return jax.shard_map(body, mesh=mesh, in_specs=in_specs, out_specs=out_specs, check_vma=False)
```

```python
import math

import jax
import jax.numpy as jnp
from jax import lax
from jax.experimental import pallas as pl
from jax.experimental.pallas import tpu as pltpu
from jax.sharding import PartitionSpec as P

HEADS = 4
EPSILON = 1e-06
BLOCK = 256
CAP = 32
F32 = jnp.float32
BF16 = jnp.bfloat16
I32 = jnp.int32


def column_of(row, size):
    pieces = []
    step = 128
    eye = lax.broadcasted_iota(I32, (step, step), 0) == lax.broadcasted_iota(I32, (step, step), 1)
    for i in range(size // step):
        part = row[:, i * step : (i + 1) * step].astype(F32)
        pieces.append(jnp.sum(jnp.where(eye, part, 0.0), axis=1, keepdims=True))
    return jnp.concatenate(pieces, axis=0)


def contract_rows(left, right):
    return lax.dot_general(left, right, (((0,), (0,)), ((), ())), preferred_element_type=F32)


def plan_order(owner_ref):
    size = owner_ref.shape[1]
    row = owner_ref[...]
    col = column_of(row, size)
    sub = lax.broadcasted_iota(I32, (size, size), 0)
    lane = lax.broadcasted_iota(I32, (size, size), 1)
    keyed = row.astype(F32)
    before = (col < keyed) | ((col == keyed) & (sub < lane))
    rank = jnp.sum(jnp.where(before, 1.0, 0.0), axis=0, keepdims=True)
    found = jnp.where(rank == sub.astype(F32), lane.astype(F32), 0.0)
    at = jnp.sum(found, axis=1, keepdims=True)
    return jnp.sum(jnp.where(sub == lane, at, 0.0), axis=0, keepdims=True).astype(I32) & (size - 1)


def plan_fetch(ids_smem, home, stage):
    def fetch(c, carry):
        for i in range(128):
            line = lax.shift_right_logical(ids_smem[c, i], 7)
            stage[c, pl.ds(i, 1), :] = home[pl.ds(line, 1), :]
        return carry

    lax.fori_loop(0, ids_smem.shape[0], fetch, 0)


def plan_requests(seq, length, ids_ref, stage, shards, rows_dev):
    seq_len = ids_ref.shape[1]
    chunk = seq_len // shards
    shift = rows_dev.bit_length() - 1
    place = lax.broadcasted_iota(I32, (128, 1), 0)
    lane = lax.broadcasted_iota(I32, (128, 128), 1)
    lane_k = lax.broadcasted_iota(I32, (128, shards), 1)
    sub = lax.broadcasted_iota(I32, (128, 128), 0)
    below = (lane < sub).astype(BF16)
    eye = lane == sub
    carry = jnp.zeros((1, shards), F32)
    lefts, rights = [], []
    owns, slots = [], []
    for b in range(seq_len // 128):
        ids = jnp.sum(
            jnp.where(eye, (ids_ref[seq : seq + 1, b * 128 : (b + 1) * 128] & 127).astype(F32), 0.0),
            axis=1,
            keepdims=True,
        )
        lines = stage[seq * (seq_len // 128) + b].astype(F32)
        home = jnp.sum(
            jnp.where(ids == lane.astype(F32), lines, 0.0), axis=1, keepdims=True
        ).astype(I32)
        at = place + b * 128
        target = jnp.where(at < length, lax.shift_right_logical(home, shift), shards)
        row = home & (rows_dev - 1)
        onehot = jnp.where(target == lane_k, 1.0, 0.0)
        onehot16 = onehot.astype(BF16)
        before = jnp.dot(below, onehot16, preferred_element_type=F32) + carry
        rank = jnp.sum(before * onehot, axis=1, keepdims=True)
        carry = carry + jnp.sum(onehot, axis=0, keepdims=True)
        at_rank = lane.astype(F32) == rank
        lefts += [onehot16, onehot16]
        rights.append(jnp.where(at_rank, (row & ~127).astype(F32), 0.0).astype(BF16))
        rights.append(jnp.where(at_rank, (row & 127).astype(F32), 0.0).astype(BF16))
        slot = jnp.where(at < length, target * CAP + rank.astype(I32), 0)
        own = jnp.where(at // chunk == lane_k, 1.0, 0.0).astype(BF16)
        at_place = lane == lax.rem(at, chunk) + CAP
        lefts += [own, own]
        rights.append(jnp.where(at_place, (slot & ~127).astype(F32), 0.0).astype(BF16))
        rights.append(jnp.where(at_place, (slot & 127).astype(F32), 0.0).astype(BF16))
    result = contract_rows(jnp.concatenate(lefts, axis=0), jnp.concatenate(rights, axis=0))
    lanes = lax.broadcasted_iota(I32, (shards, 128), 1)
    result = result.astype(I32)
    result = jnp.where(lanes < CAP, result & (rows_dev - 1), result & (shards * CAP - 1))
    return jnp.where(lanes == CAP + 16, length, result)


def exchange_kernel(
    ids_smem, len_smem, ids_ref, owner_ref, home_ref, table_ref,
    own_got, pair_got, far_got, maps_got,
    home_in, lines, asked_ref, asked_all, asked_smem, order_in, order_ref, table_in, left_in, right_in, far_in,
    own_rows, pair_rows, far_rows, stage,
    own_out, pair_out, far_out, maps_out,
    local_sem, asked_send, asked_recv, side_send, side_recv, row_send, row_recv,
):
    shards = own_got.shape[0]
    reps = 4
    seq_dev, seq_len = ids_ref.shape
    cols, rows_dev = table_ref.shape
    me = lax.axis_index("shard")
    rep = lax.axis_index("rep")
    right = lax.rem(rep + 1, reps)
    left = lax.rem(rep + reps - 1, reps)
    chunk = min(256, rows_dev)

    load = pltpu.make_async_copy(table_ref, table_in, local_sem.at[0])
    load_home = pltpu.make_async_copy(home_ref, home_in, local_sem.at[1])
    load_home.start()
    load.start()
    barrier = pltpu.get_barrier_semaphore()

    def greet(i, carry):
        peer = lax.rem(me + i, shards)
        pl.semaphore_signal(
            barrier, inc=1, device_id={"shard": peer}, device_id_type=pl.DeviceIdType.MESH
        )
        return carry

    lax.fori_loop(1, shards, greet, 0)
    for side in (left, right):
        pl.semaphore_signal(
            barrier, inc=1, device_id={"rep": side}, device_id_type=pl.DeviceIdType.MESH
        )

    eye = (
        lax.broadcasted_iota(I32, (chunk, chunk), 0) == lax.broadcasted_iota(I32, (chunk, chunk), 1)
    ).astype(BF16)

    def turn(upper, lower, rows):
        def one(c, carry):
            at = pl.multiple_of(c * chunk, chunk)
            both = jnp.concatenate([upper[:, pl.ds(at, chunk)], lower[:, pl.ds(at, chunk)]], axis=0)
            rows[pl.ds(at, chunk), :] = lax.dot_general(
                eye, both, (((1,), (1,)), ((), ())), preferred_element_type=F32
            )
            return carry

        lax.fori_loop(0, rows_dev // chunk, one, 0)

    order_in[...] = plan_order(owner_ref)
    load_home.wait()
    plan_fetch(ids_smem, home_in, lines)
    load.wait()
    pl.semaphore_wait(barrier, shards + 1)

    def side_copy(source, target, slot, side):
        return pltpu.make_async_remote_copy(
            src_ref=source,
            dst_ref=target,
            send_sem=side_send.at[slot],
            recv_sem=side_recv.at[slot],
            device_id={"rep": side},
            device_id_type=pl.DeviceIdType.MESH,
        )

    def shard_copy(source, target, send, recv, peer):
        return pltpu.make_async_remote_copy(
            src_ref=source,
            dst_ref=target,
            send_sem=send,
            recv_sem=recv,
            device_id={"shard": peer},
            device_id_type=pl.DeviceIdType.MESH,
        )

    to_right = side_copy(table_in, left_in, 0, right)
    to_left = side_copy(table_in, right_in, 1, left)
    to_right.start()
    to_left.start()
    for seq in range(seq_dev):
        length = len_smem[0, me * seq_dev + seq]
        asked_ref[:, seq, :] = plan_requests(seq, length, ids_ref, lines, shards, rows_dev)

    def ask(i, carry):
        peer = lax.rem(me + i, shards)
        shard_copy(
            asked_ref.at[peer], asked_all.at[me], asked_send, asked_recv, peer
        ).start()
        return carry

    lax.fori_loop(1, shards, ask, 0)
    keep = pltpu.make_async_copy(asked_ref.at[me], asked_all.at[me], local_sem.at[2])
    keep.start()
    spill_order = pltpu.make_async_copy(order_in, order_ref, local_sem.at[3])
    spill_order.start()
    turn(table_in, table_in, own_rows)
    keep.wait()
    spill_order.wait()
    others = pl.ds(0, shards - 1)
    shard_copy(asked_ref.at[others], asked_all.at[others], asked_send, asked_recv, me).wait()
    spill = pltpu.make_async_copy(asked_all, asked_smem, local_sem.at[4])
    spill.start()
    spill.wait()

    first_half = lax.broadcasted_iota(I32, (1, 2 * cols), 1) < cols

    def send_to(out, got, kind, peer):
        shard_copy(out.at[peer], got.at[me], row_send.at[kind], row_recv.at[kind], peer).start()

    def finish(out, got, kind):
        local = pltpu.make_async_copy(out.at[me], got.at[me], local_sem.at[5 + kind])
        local.start()
        local.wait()

    def sweep(pick, out, got, kind, paired, extra=None):
        def owner(i, carry):
            peer = lax.rem(me + i + 1, shards)
            hists = [order_ref[0, 2 * peer + q] for q in range(2)]
            if extra is not None:
                for q in range(2):
                    line = asked_all[lax.shift_right_logical(hists[q], 1)]
                    odd = lax.rem(hists[q], 2) == 1
                    extra[peer, pl.ds(q, 1), :] = jnp.where(odd, line[1:2], line[0:1])
            sources = [lax.shift_right_logical(hist, 1) for hist in hists]
            halves = [hist & 1 for hist in hists]
            slot = lax.rem(i, 2)
            if paired:
                for j in range(CAP):
                    one = pick[pl.ds(asked_smem[sources[0], halves[0], j], 1), :]
                    two = pick[pl.ds(asked_smem[sources[1], halves[1], j], 1), :]
                    stage[slot, pl.ds(j, 1), :] = jnp.where(first_half, one, two)
                out[peer] = stage[slot, :CAP, :].astype(BF16)
            else:
                for q in range(2):
                    for j in range(CAP):
                        stage[slot, pl.ds(q * CAP + j, 1), :] = pick[
                            pl.ds(asked_smem[sources[q], halves[q], j], 1), :
                        ]
                out[peer] = stage[slot].astype(BF16)

            @pl.when(i > 0)
            def _():
                before = lax.rem(me + i, shards)
                send_to(out, got, kind, before)
                if extra is not None:
                    send_to(extra, maps_got, 3, before)

            return carry

        lax.fori_loop(0, shards, owner, 0)

    sweep(own_rows, own_out, own_got, 0, True, maps_out)
    to_right.wait_recv()
    to_left.wait_recv()
    half = cols // 2
    on_right = side_copy(left_in.at[pl.ds(0, half)], far_in.at[pl.ds(0, half)], 2, right)
    on_left = side_copy(right_in.at[pl.ds(half, half)], far_in.at[pl.ds(half, half)], 3, left)
    on_right.start()
    on_left.start()
    turn(left_in, right_in, pair_rows)
    sweep(pair_rows, pair_out, pair_got, 1, False)
    on_right.wait_recv()
    on_left.wait_recv()
    turn(far_in, far_in, far_rows)
    sweep(far_rows, far_out, far_got, 2, True)
    for kind, (out, got) in enumerate(
        ((own_out, own_got), (pair_out, pair_got), (far_out, far_got), (maps_out, maps_got))
    ):
        finish(out, got, kind)
    for copy in (to_right, to_left, on_right, on_left):
        copy.wait_send()
    for kind, (out, got) in enumerate(
        ((own_out, own_got), (pair_out, pair_got), (far_out, far_got), (maps_out, maps_got))
    ):
        shard_copy(
            out.at[others], got.at[others], row_send.at[kind], row_recv.at[kind], me
        ).wait()


def exchange_rows(item_ids, lengths, owners, row_home, table, shards):
    cols, rows_dev = table.shape
    seq_dev, seq_len = item_ids.shape
    wide = 2 * cols
    any_space = pl.BlockSpec(memory_space=pl.ANY)
    smem_space = pl.BlockSpec(memory_space=pltpu.SMEM)
    vmem_space = pl.BlockSpec(memory_space=pltpu.VMEM)
    lines = seq_dev * seq_len // 128
    shapes = (
        ((shards, CAP, wide), BF16),
        ((shards, 2 * CAP, wide), BF16),
        ((shards, CAP, wide), BF16),
        ((shards, seq_dev, 128), I32),
    )
    home = row_home.reshape(-1, 128)
    return pl.pallas_call(
        exchange_kernel,
        out_shape=[jax.ShapeDtypeStruct(*shape) for shape in shapes],
        in_specs=[smem_space, smem_space, vmem_space, vmem_space, any_space, any_space],
        out_specs=[any_space] * 4,
        scratch_shapes=[
            pltpu.VMEM(home.shape, I32),
            pltpu.VMEM((lines, 128, 128), I32),
            pltpu.VMEM((shards, seq_dev, 128), I32),
            pltpu.VMEM((shards, seq_dev, 128), I32),
            pltpu.SMEM((shards, seq_dev, 128), I32),
            pltpu.VMEM(owners.shape, I32),
            pltpu.SMEM(owners.shape, I32),
            pltpu.VMEM((cols, rows_dev), BF16),
            pltpu.VMEM((cols, rows_dev), BF16),
            pltpu.VMEM((cols, rows_dev), BF16),
            pltpu.VMEM((cols, rows_dev), BF16),
            pltpu.VMEM((rows_dev, wide), F32),
            pltpu.VMEM((rows_dev, wide), F32),
            pltpu.VMEM((rows_dev, wide), F32),
            pltpu.VMEM((2, 2 * CAP, wide), F32),
            *[pltpu.VMEM(*shape) for shape in shapes],
            pltpu.SemaphoreType.DMA((9,)),
            pltpu.SemaphoreType.DMA,
            pltpu.SemaphoreType.DMA,
            pltpu.SemaphoreType.DMA((4,)),
            pltpu.SemaphoreType.DMA((4,)),
            pltpu.SemaphoreType.DMA((4,)),
            pltpu.SemaphoreType.DMA((4,)),
        ],
        compiler_params=pltpu.CompilerParams(
            collective_id=0, has_side_effects=True, vmem_limit_bytes=40 * 1024 * 1024
        ),
        name="exchange",
    )(item_ids.reshape(lines, 128), lengths, item_ids, owners, home, table)


def normed_rows(values):
    center = values - jnp.mean(values, axis=-1, keepdims=True)
    spread = jnp.mean(center * center, axis=-1, keepdims=True)
    return center * lax.rsqrt(spread + EPSILON)


def gated_linear(half):
    return half + half * jnp.tanh(half)


def layer_kernel(
    maps_ref, own_ref, pair_ref, far_ref, proj_ref, outw_ref, mixed_ref,
    flat, emb, gates, vals, quer, keys, att,
):
    seq = pl.program_id(0)
    seq_len, width = mixed_ref.shape[1:]
    head = width // HEADS
    length = maps_ref[0, seq, CAP + 16]
    rep = lax.axis_index("rep")
    shards, cap = own_ref.shape[:2]
    side = width // 4
    group = 8
    first_half = lax.broadcasted_iota(I32, (1, 2 * side), 1) < side
    swapped = seq == 1

    for r in range(4):

        @pl.when(rep == r)
        def _(r=r):
            def place_blocks(c, carry):
                span = pl.ds(c * group, group)
                rows = group * cap
                parts = {}
                for name, ref in (("own", own_ref), ("far", far_ref)):
                    part = ref[span].reshape(rows, 2 * side).astype(F32)
                    other = pltpu.roll(part, side, 1)
                    parts[name] = (
                        jnp.where(swapped, other, part),
                        jnp.where(swapped, part, other),
                    )
                pair = pair_ref[span].reshape(rows, 2 * side).astype(F32)
                turned = pltpu.roll(pair, side, 1)
                parts["left"] = (pair, turned)
                parts["right"] = (turned, pair)
                names = ("own", "right", "far", "left")
                at = pl.multiple_of(c * rows, rows)
                for tile in range(2):
                    low = parts[names[(2 * tile - r) % 4]][0]
                    high = parts[names[(2 * tile + 1 - r) % 4]][1]
                    flat[tile, pl.ds(at, rows), :] = jnp.where(first_half, low, high)
                return carry

            lax.fori_loop(0, shards // group, place_blocks, 0)

    unroll = 16

    def fetch(c, carry):
        for i in range(unroll):
            slot = maps_ref[c, seq, CAP + i]
            for tile in range(2):
                emb[tile, c, pl.ds(i, 1), :] = flat[tile, pl.ds(slot, 1), :]
        return carry

    lax.fori_loop(0, (length + unroll - 1) // unroll, fetch, 0)

    def rows_of(b):
        span = pl.ds(b * (BLOCK // unroll), BLOCK // unroll)
        return jnp.concatenate([emb[t, span].reshape(BLOCK, 2 * side) for t in range(2)], axis=1)

    blocks = (length + BLOCK - 1) // BLOCK
    place = lax.broadcasted_iota(I32, (BLOCK, 1), 0)

    def project(b, carry):
        at = pl.multiple_of(b * BLOCK, BLOCK)
        span = pl.ds(at, BLOCK)
        rows = jnp.where(place + at < length, rows_of(b), 0.0)
        normed = normed_rows(rows).astype(BF16)
        for part, ref in enumerate((gates, vals, quer, keys)):
            raw = jnp.dot(
                normed, proj_ref[:, part * width : (part + 1) * width], preferred_element_type=F32
            )
            made = gated_linear(raw * 0.5).astype(BF16)
            if part == 0:
                ref[span, :] = made
            else:
                if part == 2:
                    made = made * (0.5 / math.sqrt(head))
                for h in range(HEADS):
                    ref[h, span, :] = made[:, h * head : (h + 1) * head]
        return carry

    lax.fori_loop(0, blocks, project, 0)
    inverse = 1.0 / length.astype(F32)
    for b in range(seq_len // BLOCK):

        @pl.when(b * BLOCK < length)
        def _(b=b):
            reach = (b + 1) * BLOCK
            keep = lax.broadcasted_iota(I32, (BLOCK, BLOCK), 1) <= lax.broadcasted_iota(
                I32, (BLOCK, BLOCK), 0
            )

            def attend(h, carry):
                query = quer[h, b * BLOCK : reach, :]
                scores = lax.dot_general(
                    query, keys[h, :reach, :], (((1,), (1,)), ((), ())), preferred_element_type=F32
                )
                weights = gated_linear(scores)
                last = jnp.where(keep, weights[:, b * BLOCK :], 0.0).astype(BF16)
                if b:
                    last = jnp.concatenate([weights[:, : b * BLOCK].astype(BF16), last], axis=1)
                att[h] = jnp.dot(last, vals[h, :reach, :], preferred_element_type=F32)
                return carry

            lax.fori_loop(0, HEADS, attend, 0)
            whole = jnp.concatenate([att[h] for h in range(HEADS)], axis=1) * inverse
            gated = (normed_rows(whole) * gates[b * BLOCK : reach, :].astype(F32)).astype(BF16)
            mixed = rows_of(b) + jnp.dot(
                gated, outw_ref[...], preferred_element_type=F32
            )
            live = place + b * BLOCK < length
            mixed_ref[0, b * BLOCK : reach, :] = jnp.where(live, mixed, 0.0).astype(BF16)

        @pl.when(b * BLOCK >= length)
        def _(b=b):
            mixed_ref[0, b * BLOCK : (b + 1) * BLOCK, :] = jnp.zeros((BLOCK, width), BF16)


def layer(maps, own, pair, far, proj_weight, out_weight, seq_len):
    shards, cap, wide = own.shape
    seq_dev = 2
    width = proj_weight.shape[0]
    head = width // HEADS
    return pl.pallas_call(
        layer_kernel,
        grid=(seq_dev,),
        out_shape=jax.ShapeDtypeStruct((seq_dev, seq_len, width), BF16),
        in_specs=[
            pl.BlockSpec(memory_space=pltpu.SMEM),
            pl.BlockSpec((shards, cap, wide), lambda i: (0, 0, 0)),
            pl.BlockSpec((shards, cap, wide), lambda i: (0, i, 0)),
            pl.BlockSpec((shards, cap, wide), lambda i: (0, 0, 0)),
            pl.BlockSpec((width, 4 * width), lambda i: (0, 0)),
            pl.BlockSpec((width, width), lambda i: (0, 0)),
        ],
        out_specs=pl.BlockSpec((1, seq_len, width), lambda i: (i, 0, 0)),
        scratch_shapes=[
            pltpu.VMEM((2, shards * cap, wide), F32),
            pltpu.VMEM((2, seq_len // 16, 16, wide), F32),
            pltpu.VMEM((seq_len, width), BF16),
            pltpu.VMEM((HEADS, seq_len, head), BF16),
            pltpu.VMEM((HEADS, seq_len, head), BF16),
            pltpu.VMEM((HEADS, seq_len, head), BF16),
            pltpu.VMEM((HEADS, BLOCK, head), F32),
        ],
        compiler_params=pltpu.CompilerParams(vmem_limit_bytes=48 * 1024 * 1024),
        name="layer",
    )(maps, own, pair, far, proj_weight, out_weight)


def body(item_ids, seq_lengths, seq_owner, row_home, item_table, proj_weight, out_weight):
    shards = lax.axis_size("shard")
    seq_len = item_ids.shape[1]
    own, pair, far, maps = exchange_rows(
        item_ids, seq_lengths, seq_owner, row_home, item_table.T, shards
    )
    return layer(maps, own, pair, far, proj_weight, out_weight, seq_len)


def solution(mesh):
    in_specs = (
        P(("rep", "shard"), None),
        P("rep", None),
        P("rep", None),
        P(),
        P("shard", "rep"),
        P(),
        P(),
    )
    out_specs = P(("rep", "shard"), None, None)
    return jax.shard_map(body, mesh=mesh, in_specs=in_specs, out_specs=out_specs, check_vma=False)
```

```python
import math

import jax
import jax.numpy as jnp
from jax import lax
from jax.experimental import pallas as pl
from jax.experimental.pallas import tpu as pltpu
from jax.sharding import PartitionSpec as P

HEADS = 4
EPSILON = 1e-06
BLOCK = 256
CAP = 32
F32 = jnp.float32
BF16 = jnp.bfloat16
I32 = jnp.int32


def column_of(row, size):
    pieces = []
    step = 128
    eye = lax.broadcasted_iota(I32, (step, step), 0) == lax.broadcasted_iota(I32, (step, step), 1)
    for i in range(size // step):
        part = row[:, i * step : (i + 1) * step].astype(F32)
        pieces.append(jnp.sum(jnp.where(eye, part, 0.0), axis=1, keepdims=True))
    return jnp.concatenate(pieces, axis=0)


def contract_rows(left, right):
    return lax.dot_general(left, right, (((0,), (0,)), ((), ())), preferred_element_type=F32)


def plan_order(owner_ref):
    size = owner_ref.shape[1]
    row = owner_ref[...]
    col = column_of(row, size)
    sub = lax.broadcasted_iota(I32, (size, size), 0)
    lane = lax.broadcasted_iota(I32, (size, size), 1)
    keyed = row.astype(F32)
    before = (col < keyed) | ((col == keyed) & (sub < lane))
    rank = jnp.sum(jnp.where(before, 1.0, 0.0), axis=0, keepdims=True)
    found = jnp.where(rank == sub.astype(F32), lane.astype(F32), 0.0)
    at = jnp.sum(found, axis=1, keepdims=True)
    return jnp.sum(jnp.where(sub == lane, at, 0.0), axis=0, keepdims=True).astype(I32) & (size - 1)


def plan_fetch(ids_smem, home, stage):
    def fetch(c, carry):
        for i in range(128):
            line = lax.shift_right_logical(ids_smem[c, i], 7)
            stage[c, pl.ds(i, 1), :] = home[pl.ds(line, 1), :]
        return carry

    lax.fori_loop(0, ids_smem.shape[0], fetch, 0)


def plan_requests(seq, length, ids_ref, stage, shards, rows_dev):
    seq_len = ids_ref.shape[1]
    chunk = seq_len // shards
    shift = rows_dev.bit_length() - 1
    place = lax.broadcasted_iota(I32, (128, 1), 0)
    lane = lax.broadcasted_iota(I32, (128, 128), 1)
    lane_k = lax.broadcasted_iota(I32, (128, shards), 1)
    sub = lax.broadcasted_iota(I32, (128, 128), 0)
    below = (lane < sub).astype(BF16)
    eye = lane == sub
    carry = jnp.zeros((1, shards), F32)
    lefts, rights = [], []
    owns, slots = [], []
    for b in range(seq_len // 128):
        ids = jnp.sum(
            jnp.where(eye, (ids_ref[seq : seq + 1, b * 128 : (b + 1) * 128] & 127).astype(F32), 0.0),
            axis=1,
            keepdims=True,
        )
        lines = stage[seq * (seq_len // 128) + b].astype(F32)
        home = jnp.sum(
            jnp.where(ids == lane.astype(F32), lines, 0.0), axis=1, keepdims=True
        ).astype(I32)
        at = place + b * 128
        target = jnp.where(at < length, lax.shift_right_logical(home, shift), shards)
        row = home & (rows_dev - 1)
        onehot = jnp.where(target == lane_k, 1.0, 0.0)
        onehot16 = onehot.astype(BF16)
        before = jnp.dot(below, onehot16, preferred_element_type=F32) + carry
        rank = jnp.sum(before * onehot, axis=1, keepdims=True)
        carry = carry + jnp.sum(onehot, axis=0, keepdims=True)
        at_rank = lane.astype(F32) == rank
        lefts += [onehot16, onehot16]
        rights.append(jnp.where(at_rank, (row & ~127).astype(F32), 0.0).astype(BF16))
        rights.append(jnp.where(at_rank, (row & 127).astype(F32), 0.0).astype(BF16))
        slot = jnp.where(at < length, target * CAP + rank.astype(I32), 0)
        own = jnp.where(at // chunk == lane_k, 1.0, 0.0).astype(BF16)
        at_place = lane == lax.rem(at, chunk) + CAP
        lefts += [own, own]
        rights.append(jnp.where(at_place, (slot & ~127).astype(F32), 0.0).astype(BF16))
        rights.append(jnp.where(at_place, (slot & 127).astype(F32), 0.0).astype(BF16))
    result = contract_rows(jnp.concatenate(lefts, axis=0), jnp.concatenate(rights, axis=0))
    lanes = lax.broadcasted_iota(I32, (shards, 128), 1)
    result = result.astype(I32)
    result = jnp.where(lanes < CAP, result & (rows_dev - 1), result & (shards * CAP - 1))
    return jnp.where(lanes == CAP + 16, length, result)


def exchange_kernel(
    ids_hbm, len_hbm, owner_hbm, home_ref, table_ref,
    own_got, pair_got, far_got, maps_got,
    ids_ref, ids_lines, ids_smem, len_smem, owner_ref, home_in, lines, asked_ref, asked_all, asked_smem, order_in, order_ref, table_in, left_in, right_in, far_in,
    own_rows, pair_rows, far_rows, stage,
    own_out, pair_out, far_out, maps_out,
    local_sem, asked_send, asked_recv, side_send, side_recv, row_send, row_recv,
):
    shards = own_got.shape[0]
    reps = 4
    seq_dev, seq_len = ids_ref.shape
    cols, rows_dev = table_ref.shape
    me = lax.axis_index("shard")
    rep = lax.axis_index("rep")
    right = lax.rem(rep + 1, reps)
    left = lax.rem(rep + reps - 1, reps)
    chunk = min(256, rows_dev)

    load = pltpu.make_async_copy(table_ref, table_in, local_sem.at[0])
    load_home = pltpu.make_async_copy(home_ref, home_in, local_sem.at[1])
    load_ids = pltpu.make_async_copy(ids_hbm, ids_ref, local_sem.at[2])
    load_owner = pltpu.make_async_copy(owner_hbm, owner_ref, local_sem.at[3])
    load_len = pltpu.make_async_copy(len_hbm, len_smem, local_sem.at[4])
    load_ids.start()
    load_owner.start()
    load_len.start()
    load_home.start()
    load.start()
    barrier = pltpu.get_barrier_semaphore()

    depth = min(8, shards // 2)
    spread = shards // (2 * depth)

    def toward(i, size):
        step = (i + 1) // 2
        return lax.rem(size // 2 + step * (2 * lax.rem(i, 2) - 1) + size, size)

    def peer_at(i):
        dz = toward(i // (2 * spread), depth)
        dx = toward(lax.rem(i // 2, spread), spread)
        core = lax.rem(lax.rem(me, 2) + 1 + lax.rem(i, 2), 2)
        z = lax.rem(me // 2 + dz, depth)
        x = lax.rem(me // (2 * depth) + dx, spread)
        return (x * depth + z) * 2 + core

    def greet(i, carry):
        peer = lax.rem(me + i, shards)
        pl.semaphore_signal(
            barrier, inc=1, device_id={"shard": peer}, device_id_type=pl.DeviceIdType.MESH
        )
        return carry

    lax.fori_loop(1, shards, greet, 0)
    for side in (left, right):
        pl.semaphore_signal(
            barrier, inc=1, device_id={"rep": side}, device_id_type=pl.DeviceIdType.MESH
        )

    eye = (
        lax.broadcasted_iota(I32, (chunk, chunk), 0) == lax.broadcasted_iota(I32, (chunk, chunk), 1)
    ).astype(BF16)

    def turn(upper, lower, rows):
        def one(c, carry):
            at = pl.multiple_of(c * chunk, chunk)
            both = jnp.concatenate([upper[:, pl.ds(at, chunk)], lower[:, pl.ds(at, chunk)]], axis=0)
            rows[pl.ds(at, chunk), :] = lax.dot_general(
                eye, both, (((1,), (1,)), ((), ())), preferred_element_type=F32
            )
            return carry

        lax.fori_loop(0, rows_dev // chunk, one, 0)

    load_ids.wait()
    for seq in range(seq_dev):
        for b in range(seq_len // 128):
            at = seq * (seq_len // 128) + b
            ids_lines[at : at + 1, :] = ids_ref[seq : seq + 1, b * 128 : (b + 1) * 128]
    load_owner.wait()
    order_in[...] = plan_order(owner_ref)
    spill_ids = pltpu.make_async_copy(ids_lines, ids_smem, local_sem.at[5])
    spill_ids.start()
    spill_ids.wait()
    load_home.wait()
    plan_fetch(ids_smem, home_in, lines)
    load_len.wait()
    load.wait()
    pl.semaphore_wait(barrier, shards + 1)

    def side_copy(source, target, slot, side):
        return pltpu.make_async_remote_copy(
            src_ref=source,
            dst_ref=target,
            send_sem=side_send.at[slot],
            recv_sem=side_recv.at[slot],
            device_id={"rep": side},
            device_id_type=pl.DeviceIdType.MESH,
        )

    def shard_copy(source, target, send, recv, peer):
        return pltpu.make_async_remote_copy(
            src_ref=source,
            dst_ref=target,
            send_sem=send,
            recv_sem=recv,
            device_id={"shard": peer},
            device_id_type=pl.DeviceIdType.MESH,
        )

    to_right = side_copy(table_in, left_in, 0, right)
    to_left = side_copy(table_in, right_in, 1, left)
    to_right.start()
    to_left.start()
    for seq in range(seq_dev):
        length = len_smem[0, me * seq_dev + seq]
        asked_ref[:, seq, :] = plan_requests(seq, length, ids_ref, lines, shards, rows_dev)

    def ask(i, carry):
        peer = peer_at(i)
        shard_copy(
            asked_ref.at[peer], asked_all.at[me], asked_send, asked_recv, peer
        ).start()
        return carry

    lax.fori_loop(0, shards - 1, ask, 0)
    keep = pltpu.make_async_copy(asked_ref.at[me], asked_all.at[me], local_sem.at[6])
    keep.start()
    spill_order = pltpu.make_async_copy(order_in, order_ref, local_sem.at[7])
    spill_order.start()
    turn(table_in, table_in, own_rows)
    keep.wait()
    spill_order.wait()
    others = pl.ds(0, shards - 1)
    shard_copy(asked_ref.at[others], asked_all.at[others], asked_send, asked_recv, me).wait()
    spill = pltpu.make_async_copy(asked_all, asked_smem, local_sem.at[8])
    spill.start()
    spill.wait()

    first_half = lax.broadcasted_iota(I32, (1, 2 * cols), 1) < cols

    def send_to(out, got, kind, peer):
        shard_copy(out.at[peer], got.at[me], row_send.at[kind], row_recv.at[kind], peer).start()

    def stay(out, got, kind):
        local = pltpu.make_async_copy(out.at[me], got.at[me], local_sem.at[9 + kind])
        local.start()
        return local

    def sweep(pick, out, got, kind, paired, extra=None):
        def owner(i, carry):
            peer = peer_at(i)
            hists = [order_ref[0, 2 * peer + q] for q in range(2)]
            if extra is not None:
                for q in range(2):
                    line = asked_all[lax.shift_right_logical(hists[q], 1)]
                    odd = lax.rem(hists[q], 2) == 1
                    extra[peer, pl.ds(q, 1), :] = jnp.where(odd, line[1:2], line[0:1])
            sources = [lax.shift_right_logical(hist, 1) for hist in hists]
            halves = [hist & 1 for hist in hists]
            slot = lax.rem(i, 2)
            if paired:
                for j in range(CAP):
                    one = pick[pl.ds(asked_smem[sources[0], halves[0], j], 1), :]
                    two = pick[pl.ds(asked_smem[sources[1], halves[1], j], 1), :]
                    stage[slot, pl.ds(j, 1), :] = jnp.where(first_half, one, two)
                out[peer] = stage[slot, :CAP, :].astype(BF16)
            else:
                for q in range(2):
                    for j in range(CAP):
                        stage[slot, pl.ds(q * CAP + j, 1), :] = pick[
                            pl.ds(asked_smem[sources[q], halves[q], j], 1), :
                        ]
                out[peer] = stage[slot].astype(BF16)

            @pl.when(i > 0)
            def _():
                before = peer_at(i - 1)
                send_to(out, got, kind, before)
                if extra is not None:
                    send_to(extra, maps_got, 3, before)

            return carry

        lax.fori_loop(0, shards, owner, 0)

    sweep(own_rows, own_out, own_got, 0, True, maps_out)
    to_right.wait_recv()
    to_left.wait_recv()
    half = cols // 2
    on_right = side_copy(left_in.at[pl.ds(0, half)], far_in.at[pl.ds(0, half)], 2, right)
    on_left = side_copy(right_in.at[pl.ds(half, half)], far_in.at[pl.ds(half, half)], 3, left)
    on_right.start()
    on_left.start()
    turn(left_in, right_in, pair_rows)
    stays = [stay(own_out, own_got, 0), stay(maps_out, maps_got, 3)]
    sweep(pair_rows, pair_out, pair_got, 1, False)
    on_right.wait_recv()
    on_left.wait_recv()
    turn(far_in, far_in, far_rows)
    stays.append(stay(pair_out, pair_got, 1))
    sweep(far_rows, far_out, far_got, 2, True)
    for copy in (to_right, to_left, on_right, on_left):
        copy.wait_send()
    stays.append(stay(far_out, far_got, 2))
    for kind, (out, got) in enumerate(
        ((own_out, own_got), (pair_out, pair_got), (far_out, far_got), (maps_out, maps_got))
    ):
        shard_copy(
            out.at[others], got.at[others], row_send.at[kind], row_recv.at[kind], me
        ).wait()
    for local in stays:
        local.wait()


def exchange_rows(item_ids, lengths, owners, row_home, table, shards):
    cols, rows_dev = table.shape
    seq_dev, seq_len = item_ids.shape
    wide = 2 * cols
    any_space = pl.BlockSpec(memory_space=pl.ANY)
    hbm_space = pl.BlockSpec(memory_space=pltpu.HBM)
    lines = seq_dev * seq_len // 128
    shapes = (
        ((shards, CAP, wide), BF16),
        ((shards, 2 * CAP, wide), BF16),
        ((shards, CAP, wide), BF16),
        ((shards, seq_dev, 128), I32),
    )
    home = row_home.reshape(-1, 128)
    return pl.pallas_call(
        exchange_kernel,
        out_shape=[jax.ShapeDtypeStruct(*shape) for shape in shapes],
        in_specs=[hbm_space] * 5,
        out_specs=[any_space] * 4,
        scratch_shapes=[
            pltpu.VMEM(item_ids.shape, I32),
            pltpu.VMEM((lines, 128), I32),
            pltpu.SMEM((lines, 128), I32),
            pltpu.SMEM(lengths.shape, I32),
            pltpu.VMEM(owners.shape, I32),
            pltpu.VMEM(home.shape, I32),
            pltpu.VMEM((lines, 128, 128), I32),
            pltpu.VMEM((shards, seq_dev, 128), I32),
            pltpu.VMEM((shards, seq_dev, 128), I32),
            pltpu.SMEM((shards, seq_dev, 128), I32),
            pltpu.VMEM(owners.shape, I32),
            pltpu.SMEM(owners.shape, I32),
            pltpu.VMEM((cols, rows_dev), BF16),
            pltpu.VMEM((cols, rows_dev), BF16),
            pltpu.VMEM((cols, rows_dev), BF16),
            pltpu.VMEM((cols, rows_dev), BF16),
            pltpu.VMEM((rows_dev, wide), F32),
            pltpu.VMEM((rows_dev, wide), F32),
            pltpu.VMEM((rows_dev, wide), F32),
            pltpu.VMEM((2, 2 * CAP, wide), F32),
            *[pltpu.VMEM(*shape) for shape in shapes],
            pltpu.SemaphoreType.DMA((13,)),
            pltpu.SemaphoreType.DMA,
            pltpu.SemaphoreType.DMA,
            pltpu.SemaphoreType.DMA((4,)),
            pltpu.SemaphoreType.DMA((4,)),
            pltpu.SemaphoreType.DMA((4,)),
            pltpu.SemaphoreType.DMA((4,)),
        ],
        compiler_params=pltpu.CompilerParams(
            collective_id=0, has_side_effects=True, vmem_limit_bytes=60 * 1024 * 1024
        ),
        name="exchange",
    )(item_ids, lengths, owners, home, table)


def normed_rows(values):
    center = values - jnp.mean(values, axis=-1, keepdims=True)
    spread = jnp.mean(center * center, axis=-1, keepdims=True)
    return center * lax.rsqrt(spread + EPSILON)


def gated_linear(half):
    return half + half * jnp.tanh(half)


def layer_kernel(
    maps_hbm, own_hbm, pair_hbm, far_hbm, proj_hbm, outw_hbm, mixed_hbm,
    maps_ref, own_ref, pair_ref, far_ref, proj_ref, outw_ref,
    flat, emb, gates, vals, quer, keys, att, mixed_ref, in_sem, out_sem,
):
    seq_dev, seq_len, width = mixed_hbm.shape
    loads = [
        pltpu.make_async_copy(source, target, in_sem.at[i])
        for i, (source, target) in enumerate(
            (
                (maps_hbm, maps_ref), (own_hbm, own_ref), (pair_hbm, pair_ref),
                (far_hbm, far_ref), (proj_hbm, proj_ref), (outw_hbm, outw_ref),
            )
        )
    ]
    for load in loads:
        load.start()
    for load in loads:
        load.wait()

    def history(seq, carry):
        layer_history(
            seq, maps_ref, own_ref, pair_ref, far_ref, proj_ref, outw_ref, mixed_hbm,
            flat, emb, gates, vals, quer, keys, att, mixed_ref, out_sem,
        )
        return carry

    lax.fori_loop(0, seq_dev, history, 0)
    for seq in range(seq_dev):
        for b in range(seq_len // BLOCK):
            store_block(seq, b, mixed_ref, mixed_hbm, out_sem).wait()


def store_block(seq, b, mixed_ref, mixed_hbm, out_sem):
    span = pl.ds(b * BLOCK, BLOCK)
    return pltpu.make_async_copy(
        mixed_ref.at[seq, span], mixed_hbm.at[seq, span], out_sem.at[seq, b]
    )


def layer_history(
    seq, maps_ref, own_ref, pair_ref, far_ref, proj_ref, outw_ref, mixed_hbm,
    flat, emb, gates, vals, quer, keys, att, mixed_ref, out_sem,
):
    seq_len, width = mixed_hbm.shape[1:]
    head = width // HEADS
    length = maps_ref[0, seq, CAP + 16]
    rep = lax.axis_index("rep")
    shards, cap = own_ref.shape[:2]
    side = width // 4
    group = 8
    first_half = lax.broadcasted_iota(I32, (1, 2 * side), 1) < side
    swapped = seq == 1

    for r in range(4):

        @pl.when(rep == r)
        def _(r=r):
            def place_blocks(c, carry):
                span = pl.ds(c * group, group)
                rows = group * cap
                parts = {}
                for name, ref in (("own", own_ref), ("far", far_ref)):
                    part = ref[span].reshape(rows, 2 * side).astype(F32)
                    other = pltpu.roll(part, side, 1)
                    parts[name] = (
                        jnp.where(swapped, other, part),
                        jnp.where(swapped, part, other),
                    )
                pair = pair_ref[span, pl.ds(seq * cap, cap), :].reshape(rows, 2 * side).astype(F32)
                turned = pltpu.roll(pair, side, 1)
                parts["left"] = (pair, turned)
                parts["right"] = (turned, pair)
                names = ("own", "right", "far", "left")
                at = pl.multiple_of(c * rows, rows)
                for tile in range(2):
                    low = parts[names[(2 * tile - r) % 4]][0]
                    high = parts[names[(2 * tile + 1 - r) % 4]][1]
                    flat[tile, pl.ds(at, rows), :] = jnp.where(first_half, low, high)
                return carry

            lax.fori_loop(0, shards // group, place_blocks, 0)

    unroll = 16

    def fetch(c, carry):
        for i in range(unroll):
            slot = maps_ref[c, seq, CAP + i]
            for tile in range(2):
                emb[tile, c, pl.ds(i, 1), :] = flat[tile, pl.ds(slot, 1), :]
        return carry

    lax.fori_loop(0, (length + unroll - 1) // unroll, fetch, 0)

    def rows_of(b):
        span = pl.ds(b * (BLOCK // unroll), BLOCK // unroll)
        return jnp.concatenate([emb[t, span].reshape(BLOCK, 2 * side) for t in range(2)], axis=1)

    blocks = (length + BLOCK - 1) // BLOCK
    place = lax.broadcasted_iota(I32, (BLOCK, 1), 0)

    def project(b, carry):
        at = pl.multiple_of(b * BLOCK, BLOCK)
        span = pl.ds(at, BLOCK)
        rows = jnp.where(place + at < length, rows_of(b), 0.0)
        normed = normed_rows(rows).astype(BF16)
        for part, ref in enumerate((gates, vals, quer, keys)):
            raw = jnp.dot(
                normed, proj_ref[:, part * width : (part + 1) * width], preferred_element_type=F32
            )
            made = gated_linear(raw * 0.5).astype(BF16)
            if part == 0:
                ref[span, :] = made
            else:
                if part == 2:
                    made = made * (0.5 / math.sqrt(head))
                for h in range(HEADS):
                    ref[h, span, :] = made[:, h * head : (h + 1) * head]
        return carry

    lax.fori_loop(0, blocks, project, 0)
    inverse = 1.0 / length.astype(F32)
    for b in range(seq_len // BLOCK):

        @pl.when(b * BLOCK < length)
        def _(b=b):
            reach = (b + 1) * BLOCK
            keep = lax.broadcasted_iota(I32, (BLOCK, BLOCK), 1) <= lax.broadcasted_iota(
                I32, (BLOCK, BLOCK), 0
            )

            def attend(h, carry):
                query = quer[h, b * BLOCK : reach, :]
                scores = lax.dot_general(
                    query, keys[h, :reach, :], (((1,), (1,)), ((), ())), preferred_element_type=F32
                )
                weights = gated_linear(scores)
                last = jnp.where(keep, weights[:, b * BLOCK :], 0.0).astype(BF16)
                if b:
                    last = jnp.concatenate([weights[:, : b * BLOCK].astype(BF16), last], axis=1)
                att[h] = jnp.dot(last, vals[h, :reach, :], preferred_element_type=F32)
                return carry

            lax.fori_loop(0, HEADS, attend, 0)
            whole = jnp.concatenate([att[h] for h in range(HEADS)], axis=1) * inverse
            gated = (normed_rows(whole) * gates[b * BLOCK : reach, :].astype(F32)).astype(BF16)
            mixed = rows_of(b) + jnp.dot(
                gated, outw_ref[...], preferred_element_type=F32
            )
            live = place + b * BLOCK < length
            mixed_ref[seq, b * BLOCK : reach, :] = jnp.where(live, mixed, 0.0).astype(BF16)

        @pl.when(b * BLOCK >= length)
        def _(b=b):
            mixed_ref[seq, b * BLOCK : (b + 1) * BLOCK, :] = jnp.zeros((BLOCK, width), BF16)

        store_block(seq, b, mixed_ref, mixed_hbm, out_sem).start()


def layer(maps, own, pair, far, proj_weight, out_weight, seq_len):
    shards, cap, wide = own.shape
    seq_dev = 2
    width = proj_weight.shape[0]
    head = width // HEADS
    return pl.pallas_call(
        layer_kernel,
        out_shape=jax.ShapeDtypeStruct((seq_dev, seq_len, width), BF16),
        in_specs=[pl.BlockSpec(memory_space=pltpu.HBM)] * 6,
        out_specs=pl.BlockSpec(memory_space=pltpu.HBM),
        scratch_shapes=[
            pltpu.SMEM(maps.shape, I32),
            pltpu.VMEM(own.shape, BF16),
            pltpu.VMEM(pair.shape, BF16),
            pltpu.VMEM(far.shape, BF16),
            pltpu.VMEM(proj_weight.shape, BF16),
            pltpu.VMEM(out_weight.shape, BF16),
            pltpu.VMEM((2, shards * cap, wide), F32),
            pltpu.VMEM((2, seq_len // 16, 16, wide), F32),
            pltpu.VMEM((seq_len, width), BF16),
            pltpu.VMEM((HEADS, seq_len, head), BF16),
            pltpu.VMEM((HEADS, seq_len, head), BF16),
            pltpu.VMEM((HEADS, seq_len, head), BF16),
            pltpu.VMEM((HEADS, BLOCK, head), F32),
            pltpu.VMEM((seq_dev, seq_len, width), BF16),
            pltpu.SemaphoreType.DMA((6,)),
            pltpu.SemaphoreType.DMA((seq_dev, seq_len // BLOCK)),
        ],
        compiler_params=pltpu.CompilerParams(vmem_limit_bytes=60 * 1024 * 1024),
        name="layer",
    )(maps, own, pair, far, proj_weight, out_weight)


def body(item_ids, seq_lengths, seq_owner, row_home, item_table, proj_weight, out_weight):
    shards = lax.axis_size("shard")
    seq_len = item_ids.shape[1]
    own, pair, far, maps = exchange_rows(
        item_ids, seq_lengths, seq_owner, row_home, item_table.T, shards
    )
    return layer(maps, own, pair, far, proj_weight, out_weight, seq_len)


def solution(mesh):
    in_specs = (
        P(("rep", "shard"), None),
        P("rep", None),
        P("rep", None),
        P(),
        P("shard", "rep"),
        P(),
        P(),
    )
    out_specs = P(("rep", "shard"), None, None)
    return jax.shard_map(body, mesh=mesh, in_specs=in_specs, out_specs=out_specs, check_vma=False)
```

```python
import math

import jax
import jax.numpy as jnp
from jax import lax
from jax.experimental import pallas as pl
from jax.experimental.pallas import tpu as pltpu
from jax.sharding import PartitionSpec as P

HEADS = 4
EPSILON = 1e-06
BLOCK = 256
CAP = 32
F32 = jnp.float32
BF16 = jnp.bfloat16
I32 = jnp.int32


def column_of(row, size):
    pieces = []
    step = 128
    eye = lax.broadcasted_iota(I32, (step, step), 0) == lax.broadcasted_iota(I32, (step, step), 1)
    for i in range(size // step):
        part = row[:, i * step : (i + 1) * step].astype(F32)
        pieces.append(jnp.sum(jnp.where(eye, part, 0.0), axis=1, keepdims=True))
    return jnp.concatenate(pieces, axis=0)


def contract_rows(left, right):
    return lax.dot_general(left, right, (((0,), (0,)), ((), ())), preferred_element_type=F32)


def plan_order(owner_ref, len_ref):
    size = owner_ref.shape[1]
    row = owner_ref[...]
    col = column_of(row, size)
    row_len = len_ref[...].astype(F32)
    col_len = column_of(len_ref[...], size)
    sub = lax.broadcasted_iota(I32, (size, size), 0)
    lane = lax.broadcasted_iota(I32, (size, size), 1)
    keyed = row.astype(F32)
    sooner = (col_len > row_len) | ((col_len == row_len) & (sub < lane))
    before = (col < keyed) | ((col == keyed) & sooner)
    rank = jnp.sum(jnp.where(before, 1.0, 0.0), axis=0, keepdims=True)
    found = jnp.where(rank == sub.astype(F32), lane.astype(F32), 0.0)
    at = jnp.sum(found, axis=1, keepdims=True)
    return jnp.sum(jnp.where(sub == lane, at, 0.0), axis=0, keepdims=True).astype(I32) & (size - 1)


def plan_fetch(ids_smem, home, stage):
    def fetch(c, carry):
        for i in range(128):
            line = lax.shift_right_logical(ids_smem[c, i], 7)
            stage[c, pl.ds(i, 1), :] = home[pl.ds(line, 1), :]
        return carry

    lax.fori_loop(0, ids_smem.shape[0], fetch, 0)


def plan_requests(seq, length, index, ids_ref, stage, shards, rows_dev):
    seq_len = ids_ref.shape[1]
    chunk = seq_len // shards
    shift = rows_dev.bit_length() - 1
    place = lax.broadcasted_iota(I32, (128, 1), 0)
    lane = lax.broadcasted_iota(I32, (128, 128), 1)
    lane_k = lax.broadcasted_iota(I32, (128, shards), 1)
    sub = lax.broadcasted_iota(I32, (128, 128), 0)
    below = (lane < sub).astype(BF16)
    eye = lane == sub
    carry = jnp.zeros((1, shards), F32)
    lefts, rights = [], []
    owns, slots = [], []
    for b in range(seq_len // 128):
        ids = jnp.sum(
            jnp.where(eye, (ids_ref[seq : seq + 1, b * 128 : (b + 1) * 128] & 127).astype(F32), 0.0),
            axis=1,
            keepdims=True,
        )
        lines = stage[seq * (seq_len // 128) + b].astype(F32)
        home = jnp.sum(
            jnp.where(ids == lane.astype(F32), lines, 0.0), axis=1, keepdims=True
        ).astype(I32)
        at = place + b * 128
        target = jnp.where(at < length, lax.shift_right_logical(home, shift), shards)
        row = home & (rows_dev - 1)
        onehot = jnp.where(target == lane_k, 1.0, 0.0)
        onehot16 = onehot.astype(BF16)
        before = jnp.dot(below, onehot16, preferred_element_type=F32) + carry
        rank = jnp.sum(before * onehot, axis=1, keepdims=True)
        carry = carry + jnp.sum(onehot, axis=0, keepdims=True)
        at_rank = lane.astype(F32) == rank
        lefts += [onehot16, onehot16]
        rights.append(jnp.where(at_rank, (row & ~127).astype(F32), 0.0).astype(BF16))
        rights.append(jnp.where(at_rank, (row & 127).astype(F32), 0.0).astype(BF16))
        slot = jnp.where(at < length, target * CAP + rank.astype(I32), 0)
        own = jnp.where(at // chunk == lane_k, 1.0, 0.0).astype(BF16)
        at_place = lane == lax.rem(at, chunk) + CAP
        lefts += [own, own]
        rights.append(jnp.where(at_place, (slot & ~127).astype(F32), 0.0).astype(BF16))
        rights.append(jnp.where(at_place, (slot & 127).astype(F32), 0.0).astype(BF16))
    result = contract_rows(jnp.concatenate(lefts, axis=0), jnp.concatenate(rights, axis=0))
    lanes = lax.broadcasted_iota(I32, (shards, 128), 1)
    result = result.astype(I32)
    result = jnp.where(lanes < CAP, result & (rows_dev - 1), result & (shards * CAP - 1))
    result = jnp.where(lanes == CAP + 16, length, result)
    return jnp.where(lanes == CAP + 17, index, result)


def exchange_kernel(
    ids_hbm, len_hbm, owner_hbm, home_ref, table_ref, proj_hbm, outw_hbm,
    own_hbm, late_got, far_hbm, maps_hbm, first_hbm,
    ids_ref, ids_lines, ids_smem, len_smem, len_ref, owner_ref, home_in, lines, asked_ref, asked_all, asked_smem, order_in, order_ref, table_in, left_in, right_in, far_in,
    own_rows, pair_rows, far_rows, stage,
    own_out, pair_out, far_out, maps_out, late_out,
    own_got, pair_got, far_got, maps_got, maps_smem, proj_ref, outw_ref,
    flat, emb, gates, vals, quer, keys, att, mixed_ref, out_sem, local_sem, asked_send, asked_recv, side_send, side_recv, row_send, row_recv,
):
    shards = own_got.shape[0]
    reps = 4
    seq_dev, seq_len = ids_ref.shape
    cols, rows_dev = table_ref.shape
    me = lax.axis_index("shard")
    rep = lax.axis_index("rep")
    right = lax.rem(rep + 1, reps)
    left = lax.rem(rep + reps - 1, reps)
    chunk = min(256, rows_dev)

    load = pltpu.make_async_copy(table_ref, table_in, local_sem.at[0])
    load_home = pltpu.make_async_copy(home_ref, home_in, local_sem.at[1])
    load_ids = pltpu.make_async_copy(ids_hbm, ids_ref, local_sem.at[2])
    load_owner = pltpu.make_async_copy(owner_hbm, owner_ref, local_sem.at[3])
    load_len = pltpu.make_async_copy(len_hbm, len_smem, local_sem.at[4])
    load_lens = pltpu.make_async_copy(len_hbm, len_ref, local_sem.at[13])
    load_proj = pltpu.make_async_copy(proj_hbm, proj_ref, local_sem.at[14])
    load_outw = pltpu.make_async_copy(outw_hbm, outw_ref, local_sem.at[15])
    load_lens.start()
    load_ids.start()
    load_owner.start()
    load_len.start()
    load_home.start()
    load.start()
    barrier = pltpu.get_barrier_semaphore()

    depth = min(8, shards // 2)
    spread = shards // (2 * depth)

    def toward(i, size):
        step = (i + 1) // 2
        return lax.rem(size // 2 + step * (2 * lax.rem(i, 2) - 1) + size, size)

    def peer_at(i):
        dz = toward(i // (2 * spread), depth)
        dx = toward(lax.rem(i // 2, spread), spread)
        core = lax.rem(lax.rem(me, 2) + 1 + lax.rem(i, 2), 2)
        z = lax.rem(me // 2 + dz, depth)
        x = lax.rem(me // (2 * depth) + dx, spread)
        return (x * depth + z) * 2 + core

    def greet(i, carry):
        peer = lax.rem(me + i, shards)
        pl.semaphore_signal(
            barrier, inc=1, device_id={"shard": peer}, device_id_type=pl.DeviceIdType.MESH
        )
        return carry

    lax.fori_loop(1, shards, greet, 0)
    for side in (left, right):
        pl.semaphore_signal(
            barrier, inc=1, device_id={"rep": side}, device_id_type=pl.DeviceIdType.MESH
        )

    eye = (
        lax.broadcasted_iota(I32, (chunk, chunk), 0) == lax.broadcasted_iota(I32, (chunk, chunk), 1)
    ).astype(BF16)

    def turn(upper, lower, rows):
        def one(c, carry):
            at = pl.multiple_of(c * chunk, chunk)
            both = jnp.concatenate([upper[:, pl.ds(at, chunk)], lower[:, pl.ds(at, chunk)]], axis=0)
            rows[pl.ds(at, chunk), :] = lax.dot_general(
                eye, both, (((1,), (1,)), ((), ())), preferred_element_type=F32
            )
            return carry

        lax.fori_loop(0, rows_dev // chunk, one, 0)

    load_ids.wait()
    for seq in range(seq_dev):
        for b in range(seq_len // 128):
            at = seq * (seq_len // 128) + b
            ids_lines[at : at + 1, :] = ids_ref[seq : seq + 1, b * 128 : (b + 1) * 128]
    load_owner.wait()
    load_lens.wait()
    load_proj.start()
    load_outw.start()
    order_in[...] = plan_order(owner_ref, len_ref)
    spill_ids = pltpu.make_async_copy(ids_lines, ids_smem, local_sem.at[5])
    spill_ids.start()
    spill_ids.wait()
    load_home.wait()
    plan_fetch(ids_smem, home_in, lines)
    load_len.wait()
    load.wait()
    pl.semaphore_wait(barrier, shards + 1)

    def side_copy(source, target, slot, side):
        return pltpu.make_async_remote_copy(
            src_ref=source,
            dst_ref=target,
            send_sem=side_send.at[slot],
            recv_sem=side_recv.at[slot],
            device_id={"rep": side},
            device_id_type=pl.DeviceIdType.MESH,
        )

    def shard_copy(source, target, send, recv, peer):
        return pltpu.make_async_remote_copy(
            src_ref=source,
            dst_ref=target,
            send_sem=send,
            recv_sem=recv,
            device_id={"shard": peer},
            device_id_type=pl.DeviceIdType.MESH,
        )

    to_right = side_copy(table_in, left_in, 0, right)
    to_left = side_copy(table_in, right_in, 1, left)
    to_right.start()
    to_left.start()
    for seq in range(seq_dev):
        index = me * seq_dev + seq
        length = len_smem[0, index]
        asked_ref[:, seq, :] = plan_requests(
            seq, length, index, ids_ref, lines, shards, rows_dev
        )

    def ask(i, carry):
        peer = peer_at(i)
        shard_copy(
            asked_ref.at[peer], asked_all.at[me], asked_send, asked_recv, peer
        ).start()
        return carry

    lax.fori_loop(0, shards - 1, ask, 0)
    keep = pltpu.make_async_copy(asked_ref.at[me], asked_all.at[me], local_sem.at[6])
    keep.start()
    spill_order = pltpu.make_async_copy(order_in, order_ref, local_sem.at[7])
    spill_order.start()
    turn(table_in, table_in, own_rows)
    keep.wait()
    spill_order.wait()
    others = pl.ds(0, shards - 1)
    shard_copy(asked_ref.at[others], asked_all.at[others], asked_send, asked_recv, me).wait()
    spill = pltpu.make_async_copy(asked_all, asked_smem, local_sem.at[8])
    spill.start()
    spill.wait()

    first_half = lax.broadcasted_iota(I32, (1, 2 * cols), 1) < cols

    def send_to(out, got, kind, peer):
        shard_copy(out.at[peer], got.at[me], row_send.at[kind], row_recv.at[kind], peer).start()

    def stay(out, got, kind):
        local = pltpu.make_async_copy(out.at[me], got.at[me], local_sem.at[9 + kind])
        local.start()
        return local

    def sweep(pick, out, got, kind, of, extra=None):
        def owner(i, carry):
            peer = peer_at(i)
            hists = [order_ref[0, 2 * peer + q] for q in range(2)]
            if extra is not None:
                for q in range(2):
                    line = asked_all[lax.shift_right_logical(hists[q], 1)]
                    odd = lax.rem(hists[q], 2) == 1
                    extra[peer, pl.ds(q, 1), :] = jnp.where(odd, line[1:2], line[0:1])
            sources = [lax.shift_right_logical(hist, 1) for hist in hists]
            halves = [hist & 1 for hist in hists]
            slot = lax.rem(i, 2)
            if len(of) == 2:
                for j in range(CAP):
                    one = pick[pl.ds(asked_smem[sources[0], halves[0], j], 1), :]
                    two = pick[pl.ds(asked_smem[sources[1], halves[1], j], 1), :]
                    stage[slot, pl.ds(j, 1), :] = jnp.where(first_half, one, two)
                out[peer] = stage[slot, :CAP, :].astype(BF16)
            else:
                q = of[0]
                for j in range(CAP):
                    stage[slot, pl.ds(j, 1), :] = pick[
                        pl.ds(asked_smem[sources[q], halves[q], j], 1), :
                    ]
                out[peer] = stage[slot, :CAP, :].astype(BF16)

            @pl.when(i > 0)
            def _():
                before = peer_at(i - 1)
                send_to(out, got, kind, before)
                if extra is not None:
                    send_to(extra, maps_got, 3, before)

            return carry

        lax.fori_loop(0, shards, owner, 0)

    sweep(own_rows, own_out, own_got, 0, (0, 1), maps_out)
    to_right.wait_recv()
    to_left.wait_recv()
    half = cols // 2
    on_right = side_copy(left_in.at[pl.ds(0, half)], far_in.at[pl.ds(0, half)], 2, right)
    on_left = side_copy(right_in.at[pl.ds(half, half)], far_in.at[pl.ds(half, half)], 3, left)
    on_right.start()
    on_left.start()
    turn(left_in, right_in, pair_rows)
    stays = [stay(own_out, own_got, 0), stay(maps_out, maps_got, 3)]
    sweep(pair_rows, pair_out, pair_got, 1, (0,))
    on_right.wait_recv()
    on_left.wait_recv()
    turn(far_in, far_in, far_rows)
    stays.append(stay(pair_out, pair_got, 1))
    sweep(far_rows, far_out, far_got, 2, (0, 1))
    sweep(pair_rows, late_out, late_got, 4, (1,))
    stays.append(stay(far_out, far_got, 2))
    for local in stays:
        local.wait()
    late_stay = stay(late_out, late_got, 7)
    pairs = {
        0: (own_out, own_got),
        1: (pair_out, pair_got),
        2: (far_out, far_got),
        3: (maps_out, maps_got),
        4: (late_out, late_got),
    }

    def shared(kind):
        out, got = pairs[kind]
        return shard_copy(
            out.at[others], got.at[others], row_send.at[kind], row_recv.at[kind], me
        )

    for kind in (3, 0, 1, 2):
        shared(kind).wait_recv()
    kept = [
        pltpu.make_async_copy(source, target, local_sem.at[17 + i])
        for i, (source, target) in enumerate(
            ((maps_got, maps_smem), (maps_got, maps_hbm), (own_got, own_hbm), (far_got, far_hbm))
        )
    ]
    for copy in kept:
        copy.start()
    kept[0].wait()
    load_proj.wait()
    load_outw.wait()

    def put(b):
        return store_block(b, mixed_ref, first_hbm, out_sem)

    layer_history(
        0, True, maps_smem, own_got, pair_got, far_got, proj_ref, outw_ref, put,
        flat, emb, gates, vals, quer, keys, att, mixed_ref,
    )
    for b in range(seq_len // BLOCK):
        put(b).wait()
    for copy in kept[1:]:
        copy.wait()
    late_stay.wait()
    shared(4).wait_recv()
    for copy in (to_right, to_left, on_right, on_left):
        copy.wait_send()
    for kind in range(5):
        shared(kind).wait_send()


def layer_scratch(seq_len, width, slots):
    head = width // HEADS
    wide = width // 2
    return [
        pltpu.VMEM((2, slots, wide), F32),
        pltpu.VMEM((2, seq_len // 16, 16, wide), F32),
        pltpu.VMEM((seq_len, width), BF16),
        pltpu.VMEM((HEADS, seq_len, head), BF16),
        pltpu.VMEM((HEADS, seq_len, head), BF16),
        pltpu.VMEM((HEADS, seq_len, head), BF16),
        pltpu.VMEM((HEADS, BLOCK, head), F32),
        pltpu.VMEM((seq_len, width), BF16),
        pltpu.SemaphoreType.DMA((seq_len // BLOCK,)),
    ]


def exchange_rows(
    item_ids, lengths, owners, row_home, table, proj_weight, out_weight, shards
):
    cols, rows_dev = table.shape
    seq_dev, seq_len = item_ids.shape
    wide = 2 * cols
    any_space = pl.BlockSpec(memory_space=pl.ANY)
    hbm_space = pl.BlockSpec(memory_space=pltpu.HBM)
    lines = seq_dev * seq_len // 128
    block = ((shards, CAP, wide), BF16)
    maps = ((shards, seq_dev, 128), I32)
    width = proj_weight.shape[0]
    outs = (block, block, block, maps, ((seq_len, width), BF16))
    home = row_home.reshape(-1, 128)
    return pl.pallas_call(
        exchange_kernel,
        out_shape=[jax.ShapeDtypeStruct(*shape) for shape in outs],
        in_specs=[hbm_space] * 7,
        out_specs=[any_space] * 5,
        scratch_shapes=[
            pltpu.VMEM(item_ids.shape, I32),
            pltpu.VMEM((lines, 128), I32),
            pltpu.SMEM((lines, 128), I32),
            pltpu.SMEM(lengths.shape, I32),
            pltpu.VMEM(lengths.shape, I32),
            pltpu.VMEM(owners.shape, I32),
            pltpu.VMEM(home.shape, I32),
            pltpu.VMEM((lines, 128, 128), I32),
            pltpu.VMEM((shards, seq_dev, 128), I32),
            pltpu.VMEM((shards, seq_dev, 128), I32),
            pltpu.SMEM((shards, seq_dev, 128), I32),
            pltpu.VMEM(owners.shape, I32),
            pltpu.SMEM(owners.shape, I32),
            pltpu.VMEM((cols, rows_dev), BF16),
            pltpu.VMEM((cols, rows_dev), BF16),
            pltpu.VMEM((cols, rows_dev), BF16),
            pltpu.VMEM((cols, rows_dev), BF16),
            pltpu.VMEM((rows_dev, wide), F32),
            pltpu.VMEM((rows_dev, wide), F32),
            pltpu.VMEM((rows_dev, wide), F32),
            pltpu.VMEM((2, CAP, wide), F32),
            *[pltpu.VMEM(*shape) for shape in (block, block, block, maps, block)],
            *[pltpu.VMEM(*shape) for shape in (block, block, block, maps)],
            pltpu.SMEM(*maps),
            pltpu.VMEM(proj_weight.shape, BF16),
            pltpu.VMEM(out_weight.shape, BF16),
            *layer_scratch(seq_len, width, shards * CAP),
            pltpu.SemaphoreType.DMA((21,)),
            pltpu.SemaphoreType.DMA,
            pltpu.SemaphoreType.DMA,
            pltpu.SemaphoreType.DMA((4,)),
            pltpu.SemaphoreType.DMA((4,)),
            pltpu.SemaphoreType.DMA((5,)),
            pltpu.SemaphoreType.DMA((5,)),
        ],
        compiler_params=pltpu.CompilerParams(
            collective_id=0, has_side_effects=True, vmem_limit_bytes=60 * 1024 * 1024
        ),
        name="exchange",
    )(item_ids, lengths, owners, home, table, proj_weight, out_weight)


def normed_rows(values):
    center = values - jnp.mean(values, axis=-1, keepdims=True)
    spread = jnp.mean(center * center, axis=-1, keepdims=True)
    return center * lax.rsqrt(spread + EPSILON)


def gated_linear(half):
    return half + half * jnp.tanh(half)


def layer_kernel(
    maps_hbm, own_hbm, late_hbm, far_hbm, proj_hbm, outw_hbm, first_hbm, mixed_hbm,
    maps_ref, own_ref, late_ref, far_ref, proj_ref, outw_ref, first_ref,
    flat, emb, gates, vals, quer, keys, att, mixed_ref, out_sem, in_sem,
):
    seq_len = mixed_hbm.shape[1]
    loads = [
        pltpu.make_async_copy(source, target, in_sem.at[i])
        for i, (source, target) in enumerate(
            (
                (maps_hbm, maps_ref), (own_hbm, own_ref), (late_hbm, late_ref),
                (far_hbm, far_ref), (proj_hbm, proj_ref), (outw_hbm, outw_ref),
                (first_hbm, first_ref),
            )
        )
    ]
    for load in loads:
        load.start()
    for load in loads:
        load.wait()
    long_at = jnp.where(maps_ref[0, 0, CAP + 17] > maps_ref[0, 1, CAP + 17], 1, 0)
    move = pltpu.make_async_copy(first_ref, mixed_hbm.at[long_at], in_sem.at[7])
    move.start()

    def put(b):
        return store_block(b, mixed_ref, mixed_hbm.at[1 - long_at], out_sem)

    layer_history(
        1, False, maps_ref, own_ref, late_ref, far_ref, proj_ref, outw_ref, put,
        flat, emb, gates, vals, quer, keys, att, mixed_ref, move.wait,
    )
    for b in range(seq_len // BLOCK):
        put(b).wait()


def store_block(b, mixed_ref, mixed_hbm, out_sem):
    span = pl.ds(b * BLOCK, BLOCK)
    return pltpu.make_async_copy(mixed_ref.at[span], mixed_hbm.at[span], out_sem.at[b])


def layer_history(
    seq, whole, maps_ref, own_ref, pair_ref, far_ref, proj_ref, outw_ref, put,
    flat, emb, gates, vals, quer, keys, att, mixed_ref, ready=None,
):
    seq_len, width = mixed_ref.shape
    head = width // HEADS
    length = maps_ref[0, seq, CAP + 16]
    rep = lax.axis_index("rep")
    shards, cap = own_ref.shape[:2]
    side = width // 4
    group = 8
    first_half = lax.broadcasted_iota(I32, (1, 2 * side), 1) < side
    for r in range(4):

        @pl.when(rep == r)
        def _(r=r):
            def place_blocks(c, carry):
                span = pl.ds(c * group, group)
                rows = group * cap
                parts = {}
                for name, ref in (("own", own_ref), ("far", far_ref)):
                    part = ref[span].reshape(rows, 2 * side).astype(F32)
                    other = pltpu.roll(part, side, 1)
                    parts[name] = (part, other) if seq == 0 else (other, part)
                pair = pair_ref[span].reshape(rows, 2 * side).astype(F32)
                turned = pltpu.roll(pair, side, 1)
                parts["left"] = (pair, turned)
                parts["right"] = (turned, pair)
                names = ("own", "right", "far", "left")
                at = pl.multiple_of(c * rows, rows)
                for tile in range(2):
                    low = parts[names[(2 * tile - r) % 4]][0]
                    high = parts[names[(2 * tile + 1 - r) % 4]][1]
                    flat[tile, pl.ds(at, rows), :] = jnp.where(first_half, low, high)
                return carry

            lax.fori_loop(0, shards // group, place_blocks, 0)

    unroll = 16

    def fetch(c, carry):
        for i in range(unroll):
            slot = maps_ref[c, seq, CAP + i]
            for tile in range(2):
                emb[tile, c, pl.ds(i, 1), :] = flat[tile, pl.ds(slot, 1), :]
        return carry

    lax.fori_loop(0, seq_len // unroll if whole else (length + unroll - 1) // unroll, fetch, 0)

    def rows_of(b):
        span = pl.ds(b * (BLOCK // unroll), BLOCK // unroll)
        return jnp.concatenate([emb[t, span].reshape(BLOCK, 2 * side) for t in range(2)], axis=1)

    blocks = seq_len // BLOCK if whole else (length + BLOCK - 1) // BLOCK
    place = lax.broadcasted_iota(I32, (BLOCK, 1), 0)

    def project(b, carry):
        at = pl.multiple_of(b * BLOCK, BLOCK)
        span = pl.ds(at, BLOCK)
        rows = jnp.where(place + at < length, rows_of(b), 0.0)
        normed = normed_rows(rows).astype(BF16)
        for part, ref in enumerate((gates, vals, quer, keys)):
            raw = jnp.dot(
                normed, proj_ref[:, part * width : (part + 1) * width], preferred_element_type=F32
            )
            made = gated_linear(raw * 0.5).astype(BF16)
            if part == 0:
                ref[span, :] = made
            else:
                if part == 2:
                    made = made * (0.5 / math.sqrt(head))
                for h in range(HEADS):
                    ref[h, span, :] = made[:, h * head : (h + 1) * head]
        return carry

    lax.fori_loop(0, blocks, project, 0)
    inverse = 1.0 / length.astype(F32)
    if ready is not None:
        ready()
    keep = lax.broadcasted_iota(I32, (BLOCK, BLOCK), 1) <= lax.broadcasted_iota(
        I32, (BLOCK, BLOCK), 0
    )

    def run(b):
        reach = (b + 1) * BLOCK

        def attend(h, carry):
            query = quer[h, b * BLOCK : reach, :]
            scores = lax.dot_general(
                query, keys[h, :reach, :], (((1,), (1,)), ((), ())), preferred_element_type=F32
            )
            weights = gated_linear(scores)
            last = jnp.where(keep, weights[:, b * BLOCK :], 0.0).astype(BF16)
            if b:
                last = jnp.concatenate([weights[:, : b * BLOCK].astype(BF16), last], axis=1)
            att[h] = jnp.dot(last, vals[h, :reach, :], preferred_element_type=F32)
            return carry

        lax.fori_loop(0, HEADS, attend, 0)
        joined = jnp.concatenate([att[h] for h in range(HEADS)], axis=1) * inverse
        gated = (normed_rows(joined) * gates[b * BLOCK : reach, :].astype(F32)).astype(BF16)
        mixed = rows_of(b) + jnp.dot(gated, outw_ref[...], preferred_element_type=F32)
        live = place + b * BLOCK < length
        mixed_ref[b * BLOCK : reach, :] = jnp.where(live, mixed, 0.0).astype(BF16)

    for b in range(seq_len // BLOCK):
        if whole:
            run(b)
        else:
            pl.when(b * BLOCK < length)(lambda b=b: run(b))

            @pl.when(b * BLOCK >= length)
            def _(b=b):
                mixed_ref[b * BLOCK : (b + 1) * BLOCK, :] = jnp.zeros((BLOCK, width), BF16)

        put(b).start()


def layer(maps, own, late, far, first, proj_weight, out_weight):
    slots = own.shape[0] * own.shape[1]
    seq_len, width = first.shape
    return pl.pallas_call(
        layer_kernel,
        out_shape=jax.ShapeDtypeStruct((maps.shape[1], seq_len, width), BF16),
        in_specs=[pl.BlockSpec(memory_space=pltpu.HBM)] * 7,
        out_specs=pl.BlockSpec(memory_space=pltpu.HBM),
        scratch_shapes=[
            pltpu.SMEM(maps.shape, I32),
            pltpu.VMEM(own.shape, BF16),
            pltpu.VMEM(late.shape, BF16),
            pltpu.VMEM(far.shape, BF16),
            pltpu.VMEM(proj_weight.shape, BF16),
            pltpu.VMEM(out_weight.shape, BF16),
            pltpu.VMEM(first.shape, BF16),
            *layer_scratch(seq_len, width, slots),
            pltpu.SemaphoreType.DMA((8,)),
        ],
        compiler_params=pltpu.CompilerParams(vmem_limit_bytes=60 * 1024 * 1024),
        name="layer",
    )(maps, own, late, far, proj_weight, out_weight, first)


def body(item_ids, seq_lengths, seq_owner, row_home, item_table, proj_weight, out_weight):
    shards = lax.axis_size("shard")
    own, late, far, maps, first = exchange_rows(
        item_ids, seq_lengths, seq_owner, row_home, item_table.T, proj_weight, out_weight, shards
    )
    return layer(maps, own, late, far, first, proj_weight, out_weight)


def solution(mesh):
    in_specs = (
        P(("rep", "shard"), None),
        P("rep", None),
        P("rep", None),
        P(),
        P("shard", "rep"),
        P(),
        P(),
    )
    out_specs = P(("rep", "shard"), None, None)
    return jax.shard_map(body, mesh=mesh, in_specs=in_specs, out_specs=out_specs, check_vma=False)
```

```python
import math

import jax
import jax.numpy as jnp
from jax import lax
from jax.experimental import pallas as pl
from jax.experimental.pallas import tpu as pltpu
from jax.sharding import PartitionSpec as P

HEADS = 4
EPSILON = 1e-06
BLOCK = 256
CAP = 32
F32 = jnp.float32
BF16 = jnp.bfloat16
I32 = jnp.int32


def column_of(row, size):
    pieces = []
    step = 128
    eye = lax.broadcasted_iota(I32, (step, step), 0) == lax.broadcasted_iota(I32, (step, step), 1)
    for i in range(size // step):
        part = row[:, i * step : (i + 1) * step].astype(F32)
        pieces.append(jnp.sum(jnp.where(eye, part, 0.0), axis=1, keepdims=True))
    return jnp.concatenate(pieces, axis=0)


def contract_rows(left, right):
    return lax.dot_general(left, right, (((0,), (0,)), ((), ())), preferred_element_type=F32)


def plan_order(owner_ref, len_ref):
    size = owner_ref.shape[1]
    row = owner_ref[...]
    col = column_of(row, size)
    row_len = len_ref[...].astype(F32)
    col_len = column_of(len_ref[...], size)
    sub = lax.broadcasted_iota(I32, (size, size), 0)
    lane = lax.broadcasted_iota(I32, (size, size), 1)
    keyed = row.astype(F32)
    sooner = (col_len > row_len) | ((col_len == row_len) & (sub < lane))
    before = (col < keyed) | ((col == keyed) & sooner)
    rank = jnp.sum(jnp.where(before, 1.0, 0.0), axis=0, keepdims=True)
    found = jnp.where(rank == sub.astype(F32), lane.astype(F32), 0.0)
    at = jnp.sum(found, axis=1, keepdims=True)
    return jnp.sum(jnp.where(sub == lane, at, 0.0), axis=0, keepdims=True).astype(I32) & (size - 1)


def plan_fetch(ids_smem, home, stage):
    def fetch(c, carry):
        for i in range(128):
            line = lax.shift_right_logical(ids_smem[c, i], 7)
            stage[c, pl.ds(i, 1), :] = home[pl.ds(line, 1), :]
        return carry

    lax.fori_loop(0, ids_smem.shape[0], fetch, 0)


def plan_requests(seq, length, index, ids_ref, stage, shards, rows_dev):
    seq_len = ids_ref.shape[1]
    chunk = seq_len // shards
    shift = rows_dev.bit_length() - 1
    place = lax.broadcasted_iota(I32, (128, 1), 0)
    lane = lax.broadcasted_iota(I32, (128, 128), 1)
    lane_k = lax.broadcasted_iota(I32, (128, shards), 1)
    sub = lax.broadcasted_iota(I32, (128, 128), 0)
    below = (lane < sub).astype(BF16)
    eye = lane == sub
    carry = jnp.zeros((1, shards), F32)
    lefts, rights = [], []
    owns, slots = [], []
    for b in range(seq_len // 128):
        ids = jnp.sum(
            jnp.where(eye, (ids_ref[seq : seq + 1, b * 128 : (b + 1) * 128] & 127).astype(F32), 0.0),
            axis=1,
            keepdims=True,
        )
        lines = stage[seq * (seq_len // 128) + b].astype(F32)
        home = jnp.sum(
            jnp.where(ids == lane.astype(F32), lines, 0.0), axis=1, keepdims=True
        ).astype(I32)
        at = place + b * 128
        target = jnp.where(at < length, lax.shift_right_logical(home, shift), shards)
        row = home & (rows_dev - 1)
        onehot = jnp.where(target == lane_k, 1.0, 0.0)
        onehot16 = onehot.astype(BF16)
        before = jnp.dot(below, onehot16, preferred_element_type=F32) + carry
        rank = jnp.sum(before * onehot, axis=1, keepdims=True)
        carry = carry + jnp.sum(onehot, axis=0, keepdims=True)
        at_rank = lane.astype(F32) == rank
        lefts += [onehot16, onehot16]
        rights.append(jnp.where(at_rank, (row & ~127).astype(F32), 0.0).astype(BF16))
        rights.append(jnp.where(at_rank, (row & 127).astype(F32), 0.0).astype(BF16))
        slot = jnp.where(at < length, target * CAP + rank.astype(I32), 0)
        own = jnp.where(at // chunk == lane_k, 1.0, 0.0).astype(BF16)
        at_place = lane == lax.rem(at, chunk) + CAP
        lefts += [own, own]
        rights.append(jnp.where(at_place, (slot & ~127).astype(F32), 0.0).astype(BF16))
        rights.append(jnp.where(at_place, (slot & 127).astype(F32), 0.0).astype(BF16))
    result = contract_rows(jnp.concatenate(lefts, axis=0), jnp.concatenate(rights, axis=0))
    lanes = lax.broadcasted_iota(I32, (shards, 128), 1)
    result = result.astype(I32)
    result = jnp.where(lanes < CAP, result & (rows_dev - 1), result & (shards * CAP - 1))
    result = jnp.where(lanes == CAP + 16, length, result)
    return jnp.where(lanes == CAP + 17, index, result)


def exchange_kernel(
    ids_hbm, len_hbm, owner_hbm, home_ref, table_ref, proj_hbm, outw_hbm,
    late_got, maps_hbm, first_hbm,
    ids_ref, ids_lines, ids_smem, len_smem, len_ref, owner_ref, home_in, lines,
    asked_ref, asked_all, asked_smem, order_all, order_smem, table_in, rows, stage,
    soon_out, late_out, maps_out, soon_got, maps_got, maps_smem, proj_ref, outw_ref,
    flat, emb, gates, vals, quer, keys, att, mixed_ref, out_sem, local_sem,
    asked_send, asked_recv, order_send, order_recv, row_send, row_recv,
):
    shards = maps_hbm.shape[0]
    reps = asked_all.shape[0] // shards
    seq_dev, seq_len = ids_ref.shape
    cols, rows_dev = table_ref.shape
    me = lax.axis_index("shard")
    rep = lax.axis_index("rep")
    here = rep * shards + me
    chunk = min(256, rows_dev)
    half = CAP // 2

    load = pltpu.make_async_copy(table_ref, table_in, local_sem.at[0])
    load_home = pltpu.make_async_copy(home_ref, home_in, local_sem.at[1])
    load_ids = pltpu.make_async_copy(ids_hbm, ids_ref, local_sem.at[2])
    load_owner = pltpu.make_async_copy(owner_hbm, owner_ref, local_sem.at[3])
    load_len = pltpu.make_async_copy(len_hbm, len_smem, local_sem.at[4])
    load_lens = pltpu.make_async_copy(len_hbm, len_ref, local_sem.at[5])
    load_proj = pltpu.make_async_copy(proj_hbm, proj_ref, local_sem.at[6])
    load_outw = pltpu.make_async_copy(outw_hbm, outw_ref, local_sem.at[7])
    load_ids.start()
    load_owner.start()
    load_len.start()
    load_lens.start()
    load_home.start()
    load.start()
    barrier = pltpu.get_barrier_semaphore()

    depth = min(8, shards // 2)
    spread = shards // (2 * depth)

    def toward(i, size):
        step = (i + 1) // 2
        return lax.rem(size // 2 + step * (2 * lax.rem(i, 2) - 1) + size, size)

    def peer_at(i):
        dz = toward(i // (2 * spread), depth)
        dx = toward(lax.rem(i // 2, spread), spread)
        core = lax.rem(lax.rem(me, 2) + 1 + lax.rem(i, 2), 2)
        z = lax.rem(me // 2 + dz, depth)
        x = lax.rem(me // (2 * depth) + dx, spread)
        return (x * depth + z) * 2 + core

    def greet(i, carry):
        other = lax.rem(here + i, reps * shards)
        pl.semaphore_signal(
            barrier,
            inc=1,
            device_id={"rep": other // shards, "shard": lax.rem(other, shards)},
            device_id_type=pl.DeviceIdType.MESH,
        )
        return carry

    lax.fori_loop(1, reps * shards, greet, 0)

    eye = (
        lax.broadcasted_iota(I32, (chunk, chunk), 0) == lax.broadcasted_iota(I32, (chunk, chunk), 1)
    ).astype(BF16)

    def turn(c, carry):
        at = pl.multiple_of(c * chunk, chunk)
        part = table_in[:, pl.ds(at, chunk)]
        rows[pl.ds(at, chunk), :] = lax.dot_general(
            eye,
            jnp.concatenate([part, part], axis=0),
            (((1,), (1,)), ((), ())),
            preferred_element_type=F32,
        )
        return carry

    load_ids.wait()
    for seq in range(seq_dev):
        for b in range(seq_len // 128):
            at = seq * (seq_len // 128) + b
            ids_lines[at : at + 1, :] = ids_ref[seq : seq + 1, b * 128 : (b + 1) * 128]
    spill_ids = pltpu.make_async_copy(ids_lines, ids_smem, local_sem.at[8])
    spill_ids.start()
    load_owner.wait()
    load_lens.wait()
    order_all[rep] = plan_order(owner_ref, len_ref)
    spill_ids.wait()
    load_home.wait()
    plan_fetch(ids_smem, home_in, lines)
    load_len.wait()
    for seq in range(seq_dev):
        index = me * seq_dev + seq
        length = len_smem[0, index]
        asked_ref[:, seq, :] = plan_requests(
            seq, length, index, ids_ref, lines, shards, rows_dev
        )
    load.wait()
    load_proj.start()
    load_outw.start()
    pl.semaphore_wait(barrier, reps * shards - 1)

    def copy_to(source, target, send, recv, other, peer):
        return pltpu.make_async_remote_copy(
            src_ref=source,
            dst_ref=target,
            send_sem=send,
            recv_sem=recv,
            device_id={"rep": other, "shard": peer},
            device_id_type=pl.DeviceIdType.MESH,
        )

    def ask(i, carry):
        peer = peer_at(i)
        for turn_by in range(reps):
            other = lax.rem(rep + turn_by, reps)

            def go():
                copy_to(
                    asked_ref.at[peer], asked_all.at[here], asked_send, asked_recv, other, peer
                ).start()

            if turn_by == 0:
                pl.when(i < shards - 1)(go)
            else:
                go()
        return carry

    lax.fori_loop(0, shards, ask, 0)
    keep = pltpu.make_async_copy(asked_ref.at[me], asked_all.at[here], local_sem.at[9])
    keep.start()
    orders = [
        copy_to(
            order_all.at[rep],
            order_all.at[rep],
            order_send.at[i],
            order_recv.at[i],
            lax.rem(rep + 1 + i, reps),
            me,
        )
        for i in range(reps - 1)
    ]
    for copy in orders:
        copy.start()
    lax.fori_loop(0, rows_dev // chunk, turn, 0)
    keep.wait()
    for copy in orders:
        copy.wait()
    spill_order = pltpu.make_async_copy(order_all, order_smem, local_sem.at[10])
    spill_order.start()
    most = pl.ds(0, reps * shards - 1)
    others = pl.ds(0, shards - 1)
    all_asked = copy_to(asked_all.at[most], asked_all.at[most], asked_send, asked_recv, rep, me)
    all_asked.wait()
    spill = pltpu.make_async_copy(asked_all, asked_smem, local_sem.at[11])
    spill.start()
    spill_order.wait()
    spill.wait()

    first_half = lax.broadcasted_iota(I32, (1, 2 * cols), 1) < cols

    def sweep(q, out, got, maps):
        def owner(i, carry):
            peer = peer_at(i)
            slot = lax.rem(i, 2)
            if maps:
                for p in range(2):
                    hist = order_smem[rep, 0, 2 * peer + p]
                    line = asked_all[rep * shards + lax.shift_right_logical(hist, 1)]
                    odd = (hist & 1) == 1
                    maps_out[peer, pl.ds(p, 1), :] = jnp.where(odd, line[1:2], line[0:1])
            for turn_by in range(reps):
                other = lax.rem(rep + turn_by, reps)
                hist = order_smem[other, 0, 2 * peer + q]
                source = other * shards + lax.shift_right_logical(hist, 1)
                odd = hist & 1
                for j in range(half):
                    one = rows[pl.ds(asked_smem[source, odd, j], 1), :]
                    two = rows[pl.ds(asked_smem[source, odd, j + half], 1), :]
                    stage[slot, turn_by, pl.ds(j, 1), :] = jnp.where(first_half, one, two)
                out[other * shards + peer] = stage[slot, turn_by].astype(BF16)

            def send(peer, own):
                for turn_by in range(reps):
                    other = lax.rem(rep + turn_by, reps)

                    def go(other=other):
                        copy_to(
                            out.at[other * shards + peer],
                            got.at[here],
                            row_send.at[q],
                            row_recv.at[q],
                            other,
                            peer,
                        ).start()

                    if turn_by or not own:
                        go()
                if maps and not own:
                    copy_to(
                        maps_out.at[peer], maps_got.at[me], row_send.at[2], row_recv.at[2], rep, peer
                    ).start()

            pl.when(i > 0)(lambda: send(peer_at(i - 1), False))
            pl.when(i == shards - 1)(lambda: send(peer, True))
            return carry

        lax.fori_loop(0, shards, owner, 0)

    sweep(0, soon_out, soon_got, True)
    sweep(1, late_out, late_got, False)
    stays = [
        pltpu.make_async_copy(soon_out.at[here], soon_got.at[here], local_sem.at[12]),
        pltpu.make_async_copy(maps_out.at[me], maps_got.at[me], local_sem.at[13]),
        pltpu.make_async_copy(late_out.at[here], late_got.at[here], local_sem.at[14]),
    ]
    for local in stays:
        local.start()
    soon = copy_to(soon_out.at[most], soon_got.at[most], row_send.at[0], row_recv.at[0], rep, me)
    late = copy_to(late_out.at[most], late_got.at[most], row_send.at[1], row_recv.at[1], rep, me)
    mapped = copy_to(
        maps_out.at[others], maps_got.at[others], row_send.at[2], row_recv.at[2], rep, me
    )
    stays[1].wait()
    mapped.wait_recv()
    kept = [
        pltpu.make_async_copy(maps_got, maps_smem, local_sem.at[15]),
        pltpu.make_async_copy(maps_got, maps_hbm, local_sem.at[16]),
    ]
    for copy in kept:
        copy.start()
    load_proj.wait()
    load_outw.wait()
    kept[0].wait()
    stays[0].wait()
    soon.wait_recv()

    def put(b):
        return store_block(b, mixed_ref, first_hbm, out_sem)

    layer_history(
        0, True, maps_smem, soon_got, proj_ref, outw_ref, put,
        flat, emb, gates, vals, quer, keys, att, mixed_ref,
    )
    for b in range(seq_len // BLOCK):
        put(b).wait()
    kept[1].wait()
    stays[2].wait()
    late.wait_recv()
    for copy in (soon, late, mapped):
        copy.wait_send()


def layer_scratch(seq_len, width, slots):
    head = width // HEADS
    wide = width // 2
    return [
        pltpu.VMEM((2, slots, wide), F32),
        pltpu.VMEM((2, seq_len // 16, 16, wide), F32),
        pltpu.VMEM((seq_len, width), BF16),
        pltpu.VMEM((HEADS, seq_len, head), BF16),
        pltpu.VMEM((HEADS, seq_len, head), BF16),
        pltpu.VMEM((HEADS, seq_len, head), BF16),
        pltpu.VMEM((HEADS, BLOCK, head), F32),
        pltpu.VMEM((seq_len, width), BF16),
        pltpu.SemaphoreType.DMA((seq_len // BLOCK,)),
    ]


def exchange_rows(
    item_ids, lengths, owners, row_home, table, proj_weight, out_weight, shards
):
    cols, rows_dev = table.shape
    seq_dev, seq_len = item_ids.shape
    wide = 2 * cols
    any_space = pl.BlockSpec(memory_space=pl.ANY)
    hbm_space = pl.BlockSpec(memory_space=pltpu.HBM)
    lines = seq_dev * seq_len // 128
    reps = lax.axis_size("rep")
    block = ((reps * shards, CAP // 2, wide), BF16)
    maps = ((shards, seq_dev, 128), I32)
    asked = ((reps * shards, seq_dev, 128), I32)
    order = ((reps, *owners.shape), I32)
    width = proj_weight.shape[0]
    outs = (block, maps, ((seq_len, width), BF16))
    home = row_home.reshape(-1, 128)
    return pl.pallas_call(
        exchange_kernel,
        out_shape=[jax.ShapeDtypeStruct(*shape) for shape in outs],
        in_specs=[hbm_space] * 7,
        out_specs=[any_space] * 3,
        scratch_shapes=[
            pltpu.VMEM(item_ids.shape, I32),
            pltpu.VMEM((lines, 128), I32),
            pltpu.SMEM((lines, 128), I32),
            pltpu.SMEM(lengths.shape, I32),
            pltpu.VMEM(lengths.shape, I32),
            pltpu.VMEM(owners.shape, I32),
            pltpu.VMEM(home.shape, I32),
            pltpu.VMEM((lines, 128, 128), I32),
            pltpu.VMEM(*maps),
            pltpu.VMEM(*asked),
            pltpu.SMEM(*asked),
            pltpu.VMEM(*order),
            pltpu.SMEM(*order),
            pltpu.VMEM((cols, rows_dev), BF16),
            pltpu.VMEM((rows_dev, wide), F32),
            pltpu.VMEM((2, reps, CAP // 2, wide), F32),
            *[pltpu.VMEM(*shape) for shape in (block, block, maps, block, maps)],
            pltpu.SMEM(*maps),
            pltpu.VMEM(proj_weight.shape, BF16),
            pltpu.VMEM(out_weight.shape, BF16),
            *layer_scratch(seq_len, width, shards * CAP),
            pltpu.SemaphoreType.DMA((17,)),
            pltpu.SemaphoreType.DMA,
            pltpu.SemaphoreType.DMA,
            pltpu.SemaphoreType.DMA((reps - 1,)),
            pltpu.SemaphoreType.DMA((reps - 1,)),
            pltpu.SemaphoreType.DMA((3,)),
            pltpu.SemaphoreType.DMA((3,)),
        ],
        compiler_params=pltpu.CompilerParams(
            collective_id=0, has_side_effects=True, vmem_limit_bytes=60 * 1024 * 1024
        ),
        name="exchange",
    )(item_ids, lengths, owners, home, table, proj_weight, out_weight)


def normed_rows(values):
    center = values - jnp.mean(values, axis=-1, keepdims=True)
    spread = jnp.mean(center * center, axis=-1, keepdims=True)
    return center * lax.rsqrt(spread + EPSILON)


def gated_linear(half):
    return half + half * jnp.tanh(half)


def layer_kernel(
    maps_hbm, late_hbm, proj_hbm, outw_hbm, first_hbm, mixed_hbm,
    maps_ref, late_ref, proj_ref, outw_ref, first_ref,
    flat, emb, gates, vals, quer, keys, att, mixed_ref, out_sem, in_sem,
):
    seq_len = mixed_hbm.shape[1]
    loads = [
        pltpu.make_async_copy(source, target, in_sem.at[i])
        for i, (source, target) in enumerate(
            (
                (maps_hbm, maps_ref), (late_hbm, late_ref), (proj_hbm, proj_ref),
                (outw_hbm, outw_ref), (first_hbm, first_ref),
            )
        )
    ]
    for load in loads:
        load.start()
    for load in loads:
        load.wait()
    long_at = jnp.where(maps_ref[0, 0, CAP + 17] > maps_ref[0, 1, CAP + 17], 1, 0)
    move = pltpu.make_async_copy(first_ref, mixed_hbm.at[long_at], in_sem.at[7])
    move.start()

    def put(b):
        return store_block(b, mixed_ref, mixed_hbm.at[1 - long_at], out_sem)

    layer_history(
        1, False, maps_ref, late_ref, proj_ref, outw_ref, put,
        flat, emb, gates, vals, quer, keys, att, mixed_ref, move.wait,
    )
    for b in range(seq_len // BLOCK):
        put(b).wait()


def store_block(b, mixed_ref, mixed_hbm, out_sem):
    span = pl.ds(b * BLOCK, BLOCK)
    return pltpu.make_async_copy(mixed_ref.at[span], mixed_hbm.at[span], out_sem.at[b])


def layer_history(
    seq, whole, maps_ref, got_ref, proj_ref, outw_ref, put,
    flat, emb, gates, vals, quer, keys, att, mixed_ref, ready=None,
):
    seq_len, width = mixed_ref.shape
    head = width // HEADS
    length = maps_ref[0, seq, CAP + 16]
    side = width // 4
    half = got_ref.shape[1]
    shards = got_ref.shape[0] // 4
    group = 8
    first_half = lax.broadcasted_iota(I32, (1, 1, 2 * side), 2) < side

    def place_blocks(c, carry):
        rows = group * 2 * half
        at = pl.multiple_of(c * rows, rows)
        for tile in range(2):
            low, high = (
                got_ref[pl.ds((2 * tile + i) * shards + c * group, group)].astype(F32)
                for i in range(2)
            )
            upper = jnp.where(first_half, low, pltpu.roll(high, side, 2))
            lower = jnp.where(first_half, pltpu.roll(low, side, 2), high)
            flat[tile, pl.ds(at, rows), :] = jnp.concatenate([upper, lower], axis=1).reshape(
                rows, 2 * side
            )
        return carry

    lax.fori_loop(0, shards // group, place_blocks, 0)

    unroll = 16

    def fetch(c, carry):
        for i in range(unroll):
            slot = maps_ref[c, seq, CAP + i]
            for tile in range(2):
                emb[tile, c, pl.ds(i, 1), :] = flat[tile, pl.ds(slot, 1), :]
        return carry

    lax.fori_loop(0, seq_len // unroll if whole else (length + unroll - 1) // unroll, fetch, 0)

    def rows_of(b):
        span = pl.ds(b * (BLOCK // unroll), BLOCK // unroll)
        return jnp.concatenate([emb[t, span].reshape(BLOCK, 2 * side) for t in range(2)], axis=1)

    blocks = seq_len // BLOCK if whole else (length + BLOCK - 1) // BLOCK
    place = lax.broadcasted_iota(I32, (BLOCK, 1), 0)

    def project(b, carry):
        at = pl.multiple_of(b * BLOCK, BLOCK)
        span = pl.ds(at, BLOCK)
        rows = jnp.where(place + at < length, rows_of(b), 0.0)
        normed = normed_rows(rows).astype(BF16)
        for part, ref in enumerate((gates, vals, quer, keys)):
            raw = jnp.dot(
                normed, proj_ref[:, part * width : (part + 1) * width], preferred_element_type=F32
            )
            made = gated_linear(raw * 0.5).astype(BF16)
            if part == 0:
                ref[span, :] = made
            else:
                if part == 2:
                    made = made * (0.5 / math.sqrt(head))
                for h in range(HEADS):
                    ref[h, span, :] = made[:, h * head : (h + 1) * head]
        return carry

    lax.fori_loop(0, blocks, project, 0)
    inverse = 1.0 / length.astype(F32)
    if ready is not None:
        ready()
    keep = lax.broadcasted_iota(I32, (BLOCK, BLOCK), 1) <= lax.broadcasted_iota(
        I32, (BLOCK, BLOCK), 0
    )

    def run(b):
        reach = (b + 1) * BLOCK

        def attend(h, carry):
            query = quer[h, b * BLOCK : reach, :]
            scores = lax.dot_general(
                query, keys[h, :reach, :], (((1,), (1,)), ((), ())), preferred_element_type=F32
            )
            weights = gated_linear(scores)
            last = jnp.where(keep, weights[:, b * BLOCK :], 0.0).astype(BF16)
            if b:
                last = jnp.concatenate([weights[:, : b * BLOCK].astype(BF16), last], axis=1)
            att[h] = jnp.dot(last, vals[h, :reach, :], preferred_element_type=F32)
            return carry

        lax.fori_loop(0, HEADS, attend, 0)
        joined = jnp.concatenate([att[h] for h in range(HEADS)], axis=1) * inverse
        gated = (normed_rows(joined) * gates[b * BLOCK : reach, :].astype(F32)).astype(BF16)
        mixed = rows_of(b) + jnp.dot(gated, outw_ref[...], preferred_element_type=F32)
        live = place + b * BLOCK < length
        mixed_ref[b * BLOCK : reach, :] = jnp.where(live, mixed, 0.0).astype(BF16)

    for b in range(seq_len // BLOCK):
        if whole:
            run(b)
        else:
            pl.when(b * BLOCK < length)(lambda b=b: run(b))

            @pl.when(b * BLOCK >= length)
            def _(b=b):
                mixed_ref[b * BLOCK : (b + 1) * BLOCK, :] = jnp.zeros((BLOCK, width), BF16)

        put(b).start()


def layer(maps, late, first, proj_weight, out_weight):
    slots = maps.shape[0] * CAP
    seq_len, width = first.shape
    return pl.pallas_call(
        layer_kernel,
        out_shape=jax.ShapeDtypeStruct((maps.shape[1], seq_len, width), BF16),
        in_specs=[pl.BlockSpec(memory_space=pltpu.HBM)] * 5,
        out_specs=pl.BlockSpec(memory_space=pltpu.HBM),
        scratch_shapes=[
            pltpu.SMEM(maps.shape, I32),
            pltpu.VMEM(late.shape, BF16),
            pltpu.VMEM(proj_weight.shape, BF16),
            pltpu.VMEM(out_weight.shape, BF16),
            pltpu.VMEM(first.shape, BF16),
            *layer_scratch(seq_len, width, slots),
            pltpu.SemaphoreType.DMA((8,)),
        ],
        compiler_params=pltpu.CompilerParams(vmem_limit_bytes=60 * 1024 * 1024),
        name="layer",
    )(maps, late, proj_weight, out_weight, first)


def body(item_ids, seq_lengths, seq_owner, row_home, item_table, proj_weight, out_weight):
    shards = lax.axis_size("shard")
    late, maps, first = exchange_rows(
        item_ids, seq_lengths, seq_owner, row_home, item_table.T, proj_weight, out_weight, shards
    )
    return layer(maps, late, first, proj_weight, out_weight)


def solution(mesh):
    in_specs = (
        P(("rep", "shard"), None),
        P("rep", None),
        P("rep", None),
        P(),
        P("shard", "rep"),
        P(),
        P(),
    )
    out_specs = P(("rep", "shard"), None, None)
    return jax.shard_map(body, mesh=mesh, in_specs=in_specs, out_specs=out_specs, check_vma=False)
```

```python
import math

import jax
import jax.numpy as jnp
from jax import lax
from jax.experimental import pallas as pl
from jax.experimental.pallas import tpu as pltpu
from jax.sharding import PartitionSpec as P

HEADS = 4
EPSILON = 1e-06
BLOCK = 256
CAP = 32
F32 = jnp.float32
BF16 = jnp.bfloat16
I32 = jnp.int32


def column_of(row, size):
    pieces = []
    step = 128
    eye = lax.broadcasted_iota(I32, (step, step), 0) == lax.broadcasted_iota(I32, (step, step), 1)
    for i in range(size // step):
        part = row[:, i * step : (i + 1) * step].astype(F32)
        pieces.append(jnp.sum(jnp.where(eye, part, 0.0), axis=1, keepdims=True))
    return jnp.concatenate(pieces, axis=0)


def contract_rows(left, right):
    return lax.dot_general(left, right, (((0,), (0,)), ((), ())), preferred_element_type=F32)


def plan_order(owner_ref, len_ref):
    size = owner_ref.shape[1]
    row = owner_ref[...]
    col = column_of(row, size)
    row_len = len_ref[...].astype(F32)
    col_len = column_of(len_ref[...], size)
    sub = lax.broadcasted_iota(I32, (size, size), 0)
    lane = lax.broadcasted_iota(I32, (size, size), 1)
    keyed = row.astype(F32)
    sooner = (col_len > row_len) | ((col_len == row_len) & (sub < lane))
    before = (col < keyed) | ((col == keyed) & sooner)
    rank = jnp.sum(jnp.where(before, 1.0, 0.0), axis=0, keepdims=True)
    found = jnp.where(rank == sub.astype(F32), lane.astype(F32), 0.0)
    at = jnp.sum(found, axis=1, keepdims=True)
    return jnp.sum(jnp.where(sub == lane, at, 0.0), axis=0, keepdims=True).astype(I32) & (size - 1)


def plan_fetch(ids_smem, home, stage):
    def fetch(c, carry):
        for i in range(128):
            stage[c, pl.ds(i, 1), :] = home[pl.ds(ids_smem[c, i], 1), :]
        return carry

    lax.fori_loop(0, ids_smem.shape[0], fetch, 0)


def plan_requests(seq, length, index, ids_ref, stage, shards, rows_dev):
    seq_len = ids_ref.shape[1]
    chunk = seq_len // shards
    shift = rows_dev.bit_length() - 1
    place = lax.broadcasted_iota(I32, (128, 1), 0)
    lane = lax.broadcasted_iota(I32, (128, 128), 1)
    lane_k = lax.broadcasted_iota(I32, (128, shards), 1)
    sub = lax.broadcasted_iota(I32, (128, 128), 0)
    below = (lane < sub).astype(BF16)
    eye = lane == sub
    carry = jnp.zeros((1, shards), F32)
    lefts, rights = [], []
    owns, slots = [], []
    for b in range(seq_len // 128):
        ids = jnp.sum(
            jnp.where(eye, (ids_ref[seq : seq + 1, b * 128 : (b + 1) * 128] & 127).astype(F32), 0.0),
            axis=1,
            keepdims=True,
        )
        lines = stage[seq * (seq_len // 128) + b].astype(F32)
        home = jnp.sum(
            jnp.where(ids == lane.astype(F32), lines, 0.0), axis=1, keepdims=True
        ).astype(I32)
        at = place + b * 128
        target = jnp.where(at < length, lax.shift_right_logical(home, shift), shards)
        row = home & (rows_dev - 1)
        onehot = jnp.where(target == lane_k, 1.0, 0.0)
        onehot16 = onehot.astype(BF16)
        before = jnp.dot(below, onehot16, preferred_element_type=F32) + carry
        rank = jnp.sum(before * onehot, axis=1, keepdims=True)
        carry = carry + jnp.sum(onehot, axis=0, keepdims=True)
        at_rank = lane.astype(F32) == rank
        lefts += [onehot16, onehot16]
        rights.append(jnp.where(at_rank, (row & ~127).astype(F32), 0.0).astype(BF16))
        rights.append(jnp.where(at_rank, (row & 127).astype(F32), 0.0).astype(BF16))
        slot = jnp.where(at < length, target * CAP + rank.astype(I32), 0)
        own = jnp.where(at // chunk == lane_k, 1.0, 0.0).astype(BF16)
        at_place = lane == lax.rem(at, chunk) + CAP
        lefts += [own, own]
        rights.append(jnp.where(at_place, (slot & ~127).astype(F32), 0.0).astype(BF16))
        rights.append(jnp.where(at_place, (slot & 127).astype(F32), 0.0).astype(BF16))
    result = contract_rows(jnp.concatenate(lefts, axis=0), jnp.concatenate(rights, axis=0))
    lanes = lax.broadcasted_iota(I32, (shards, 128), 1)
    result = result.astype(I32)
    result = jnp.where(lanes < CAP, result & (rows_dev - 1), result & (shards * CAP - 1))
    result = jnp.where(lanes == CAP + 16, length, result)
    return jnp.where(lanes == CAP + 17, index, result)


def exchange_kernel(
    ids_hbm, len_hbm, owner_hbm, home_ref, table_ref, proj_hbm, outw_hbm,
    late_got, maps_hbm, first_hbm,
    ids_ref, ids_lines, ids_smem, len_smem, len_ref, owner_ref, home_in, lines,
    asked_ref, asked_all, asked_two, asked_smem, order_all, order_smem, table_in, rows, stage,
    soon_out, late_out, maps_out, soon_got, maps_got, maps_smem, proj_ref, outw_ref,
    flat, emb, gates, vals, quer, keys, att, mixed_ref, out_sem, local_sem,
    asked_send, asked_recv, order_send, order_recv, row_send, row_recv,
):
    shards = maps_hbm.shape[0]
    reps = asked_all.shape[0] // shards
    seq_dev, seq_len = ids_ref.shape
    cols, rows_dev = table_ref.shape
    me = lax.axis_index("shard")
    rep = lax.axis_index("rep")
    here = rep * shards + me
    chunk = min(256, rows_dev)
    half = CAP // 2

    load = pltpu.make_async_copy(table_ref, table_in, local_sem.at[0])
    load_home = pltpu.make_async_copy(home_ref, home_in, local_sem.at[1])
    load_ids = pltpu.make_async_copy(ids_hbm, ids_ref, local_sem.at[2])
    load_owner = pltpu.make_async_copy(owner_hbm, owner_ref, local_sem.at[3])
    load_len = pltpu.make_async_copy(len_hbm, len_smem, local_sem.at[4])
    load_lens = pltpu.make_async_copy(len_hbm, len_ref, local_sem.at[5])
    load_proj = pltpu.make_async_copy(proj_hbm, proj_ref, local_sem.at[6])
    load_outw = pltpu.make_async_copy(outw_hbm, outw_ref, local_sem.at[7])
    load_ids.start()
    load_owner.start()
    load_len.start()
    load_lens.start()
    load_home.start()
    load.start()
    barrier = pltpu.get_barrier_semaphore()

    depth = min(8, shards // 2)
    spread = shards // (2 * depth)

    def toward(i, size):
        step = lax.div(i + 1, 2)
        return lax.rem(size // 2 + step * (2 * lax.rem(i, 2) - 1) + size, size)

    def peer_at(i):
        dz = toward(lax.div(i, 2 * spread), depth)
        dx = toward(lax.rem(lax.div(i, 2), spread), spread)
        core = lax.rem(lax.rem(me, 2) + 1 + lax.rem(i, 2), 2)
        z = lax.rem(lax.div(me, 2) + dz, depth)
        x = lax.rem(lax.div(me, 2 * depth) + dx, spread)
        return (x * depth + z) * 2 + core

    def greet(i, carry):
        peer = lax.rem(me + i, shards)
        for turn_by in range(reps):
            def go(turn_by=turn_by):
                pl.semaphore_signal(
                    barrier,
                    inc=1,
                    device_id={"rep": lax.rem(rep + turn_by, reps), "shard": peer},
                    device_id_type=pl.DeviceIdType.MESH,
                )

            if turn_by == 0:
                pl.when(i < shards)(go)
            else:
                go()
        return carry

    lax.fori_loop(1, shards + 1, greet, 0)

    eye = (
        lax.broadcasted_iota(I32, (chunk, chunk), 0) == lax.broadcasted_iota(I32, (chunk, chunk), 1)
    ).astype(BF16)

    def turn(c, carry):
        at = pl.multiple_of(c * chunk, chunk)
        part = table_in[:, pl.ds(at, chunk)]
        rows[pl.ds(at, chunk), :] = lax.dot_general(
            eye,
            jnp.concatenate([part, part], axis=0),
            (((1,), (1,)), ((), ())),
            preferred_element_type=F32,
        )
        return carry

    load_ids.wait()
    for seq in range(seq_dev):
        for b in range(seq_len // 128):
            at = seq * (seq_len // 128) + b
            ids_lines[at : at + 1, :] = lax.shift_right_logical(
                ids_ref[seq : seq + 1, b * 128 : (b + 1) * 128], 7
            ) & (home_in.shape[0] - 1)
    spill_ids = pltpu.make_async_copy(ids_lines, ids_smem, local_sem.at[8])
    spill_ids.start()
    load_owner.wait()
    load_lens.wait()
    order_all[rep] = plan_order(owner_ref, len_ref)
    spill_ids.wait()
    load_home.wait()
    plan_fetch(ids_smem, home_in, lines)
    load_len.wait()
    parts = []
    for seq in range(seq_dev):
        index = me * seq_dev + seq
        length = len_smem[0, index]
        parts.append(plan_requests(seq, length, index, ids_ref, lines, shards, rows_dev))
    asked_ref[...] = (parts[0] + pltpu.roll(parts[1], 64, 1)).reshape(asked_ref.shape)
    load.wait()
    load_proj.start()
    load_outw.start()
    pl.semaphore_wait(barrier, reps * shards - 1)

    def copy_to(source, target, send, recv, other, peer):
        return pltpu.make_async_remote_copy(
            src_ref=source,
            dst_ref=target,
            send_sem=send,
            recv_sem=recv,
            device_id={"rep": other, "shard": peer},
            device_id_type=pl.DeviceIdType.MESH,
        )

    def ask(i, carry):
        peer = peer_at(i)
        for turn_by in range(reps):
            other = lax.rem(rep + turn_by, reps)

            def go():
                copy_to(
                    asked_ref.at[peer], asked_all.at[here], asked_send, asked_recv, other, peer
                ).start()

            if turn_by == 0:
                pl.when(i < shards - 1)(go)
            else:
                go()
        return carry

    lax.fori_loop(0, shards, ask, 0)
    keep = pltpu.make_async_copy(asked_ref.at[me], asked_all.at[here], local_sem.at[9])
    keep.start()
    orders = [
        copy_to(
            order_all.at[rep],
            order_all.at[rep],
            order_send.at[i],
            order_recv.at[i],
            lax.rem(rep + 1 + i, reps),
            me,
        )
        for i in range(reps - 1)
    ]
    for copy in orders:
        copy.start()
    lax.fori_loop(0, rows_dev // chunk, turn, 0)
    keep.wait()
    for copy in orders:
        copy.wait()
    spill_order = pltpu.make_async_copy(order_all, order_smem, local_sem.at[10])
    spill_order.start()
    most = pl.ds(0, reps * shards - 1)
    others = pl.ds(0, shards - 1)
    all_asked = copy_to(asked_all.at[most], asked_all.at[most], asked_send, asked_recv, rep, me)
    all_asked.wait()
    both = asked_all[...].reshape(reps * shards, 128)
    at_row = lax.broadcasted_iota(I32, both.shape, 1) < CAP
    for q, line in enumerate((both, pltpu.roll(both, 64, 1))):
        asked_two[q] = jnp.where(at_row, line & (rows_dev - 1), line & (shards * CAP - 1))
    spill = pltpu.make_async_copy(asked_two, asked_smem, local_sem.at[11])
    spill.start()
    spill_order.wait()
    spill.wait()

    first_half = lax.broadcasted_iota(I32, (1, 2 * cols), 1) < cols

    def sweep(q, out, got, maps):
        def owner(i, carry):
            peer = peer_at(i)
            slot = lax.rem(i, 2)
            if maps:
                for p in range(2):
                    hist = order_smem[rep, 0, 2 * peer + p]
                    at = rep * shards + lax.shift_right_logical(hist, 1)
                    maps_out[peer, pl.ds(p, 1), :] = asked_two[hist & 1, pl.ds(at, 1), :]
            for turn_by in range(reps):
                other = lax.rem(rep + turn_by, reps)
                hist = order_smem[other, 0, 2 * peer + q]
                source = other * shards + lax.shift_right_logical(hist, 1)
                odd = hist & 1
                for j in range(half):
                    one = rows[pl.ds(asked_smem[odd, source, j], 1), :]
                    two = rows[pl.ds(asked_smem[odd, source, j + half], 1), :]
                    stage[slot, turn_by, pl.ds(j, 1), :] = jnp.where(first_half, one, two)
                out[other * shards + peer] = stage[slot, turn_by].astype(BF16)

            def send(peer, own):
                for turn_by in range(reps):
                    other = lax.rem(rep + turn_by, reps)

                    def go(other=other):
                        copy_to(
                            out.at[other * shards + peer],
                            got.at[here],
                            row_send.at[q],
                            row_recv.at[q],
                            other,
                            peer,
                        ).start()

                    if turn_by or not own:
                        go()
                if maps and not own:
                    copy_to(
                        maps_out.at[peer], maps_got.at[me], row_send.at[2], row_recv.at[2], rep, peer
                    ).start()

            pl.when(i > 0)(lambda: send(peer_at(i - 1), False))
            pl.when(i == shards - 1)(lambda: send(peer, True))
            return carry

        lax.fori_loop(0, shards, owner, 0)

    sweep(0, soon_out, soon_got, True)
    sweep(1, late_out, late_got, False)
    stays = [
        pltpu.make_async_copy(soon_out.at[here], soon_got.at[here], local_sem.at[12]),
        pltpu.make_async_copy(maps_out.at[me], maps_got.at[me], local_sem.at[13]),
        pltpu.make_async_copy(late_out.at[here], late_got.at[here], local_sem.at[14]),
    ]
    for local in stays:
        local.start()
    soon = copy_to(soon_out.at[most], soon_got.at[most], row_send.at[0], row_recv.at[0], rep, me)
    late = copy_to(late_out.at[most], late_got.at[most], row_send.at[1], row_recv.at[1], rep, me)
    mapped = copy_to(
        maps_out.at[others], maps_got.at[others], row_send.at[2], row_recv.at[2], rep, me
    )
    stays[1].wait()
    mapped.wait_recv()
    kept = [
        pltpu.make_async_copy(maps_got, maps_smem, local_sem.at[15]),
        pltpu.make_async_copy(maps_got, maps_hbm, local_sem.at[16]),
    ]
    for copy in kept:
        copy.start()
    load_proj.wait()
    load_outw.wait()
    kept[0].wait()
    stays[0].wait()
    soon.wait_recv()

    def put(b):
        return store_block(b, mixed_ref, first_hbm, out_sem)

    layer_history(
        0, True, maps_smem, soon_got, proj_ref, outw_ref, put,
        flat, emb, gates, vals, quer, keys, att, mixed_ref,
    )
    for b in range(seq_len // BLOCK):
        put(b).wait()
    kept[1].wait()
    stays[2].wait()
    late.wait_recv()
    for copy in (soon, late, mapped):
        copy.wait_send()


def layer_scratch(seq_len, width, slots):
    head = width // HEADS
    wide = width // 2
    return [
        pltpu.VMEM((2, slots, wide), F32),
        pltpu.VMEM((2, seq_len // 16, 16, wide), F32),
        pltpu.VMEM((seq_len, width), BF16),
        pltpu.VMEM((HEADS, seq_len, head), BF16),
        pltpu.VMEM((HEADS, seq_len, head), BF16),
        pltpu.VMEM((HEADS, seq_len, head), BF16),
        pltpu.VMEM((HEADS, BLOCK, head), F32),
        pltpu.VMEM((seq_len, width), BF16),
        pltpu.SemaphoreType.DMA((seq_len // BLOCK,)),
    ]


def exchange_rows(
    item_ids, lengths, owners, row_home, table, proj_weight, out_weight, shards
):
    cols, rows_dev = table.shape
    seq_dev, seq_len = item_ids.shape
    wide = 2 * cols
    any_space = pl.BlockSpec(memory_space=pl.ANY)
    hbm_space = pl.BlockSpec(memory_space=pltpu.HBM)
    lines = seq_dev * seq_len // 128
    reps = lax.axis_size("rep")
    block = ((reps * shards, CAP // 2, wide), BF16)
    maps = ((shards, seq_dev, 128), I32)
    asked = ((seq_dev, reps * shards, 128), I32)
    order = ((reps, *owners.shape), I32)
    width = proj_weight.shape[0]
    outs = (block, maps, ((seq_len, width), BF16))
    home = row_home.reshape(-1, 128)
    return pl.pallas_call(
        exchange_kernel,
        out_shape=[jax.ShapeDtypeStruct(*shape) for shape in outs],
        in_specs=[hbm_space] * 7,
        out_specs=[any_space] * 3,
        scratch_shapes=[
            pltpu.VMEM(item_ids.shape, I32),
            pltpu.VMEM((lines, 128), I32),
            pltpu.SMEM((lines, 128), I32),
            pltpu.SMEM(lengths.shape, I32),
            pltpu.VMEM(lengths.shape, I32),
            pltpu.VMEM(owners.shape, I32),
            pltpu.VMEM(home.shape, I32),
            pltpu.VMEM((lines, 128, 128), I32),
            pltpu.VMEM((shards, 1, 128), I32),
            pltpu.VMEM((reps * shards, 1, 128), I32),
            pltpu.VMEM(*asked),
            pltpu.SMEM(*asked),
            pltpu.VMEM(*order),
            pltpu.SMEM(*order),
            pltpu.VMEM((cols, rows_dev), BF16),
            pltpu.VMEM((rows_dev, wide), F32),
            pltpu.VMEM((2, reps, CAP // 2, wide), F32),
            *[pltpu.VMEM(*shape) for shape in (block, block, maps, block, maps)],
            pltpu.SMEM(*maps),
            pltpu.VMEM(proj_weight.shape, BF16),
            pltpu.VMEM(out_weight.shape, BF16),
            *layer_scratch(seq_len, width, shards * CAP),
            pltpu.SemaphoreType.DMA((17,)),
            pltpu.SemaphoreType.DMA,
            pltpu.SemaphoreType.DMA,
            pltpu.SemaphoreType.DMA((reps - 1,)),
            pltpu.SemaphoreType.DMA((reps - 1,)),
            pltpu.SemaphoreType.DMA((3,)),
            pltpu.SemaphoreType.DMA((3,)),
        ],
        compiler_params=pltpu.CompilerParams(
            collective_id=0, has_side_effects=True, vmem_limit_bytes=60 * 1024 * 1024
        ),
        name="exchange",
    )(item_ids, lengths, owners, home, table, proj_weight, out_weight)


def normed_rows(values):
    center = values - jnp.mean(values, axis=-1, keepdims=True)
    spread = jnp.mean(center * center, axis=-1, keepdims=True)
    return center * lax.rsqrt(spread + EPSILON)


def gated_linear(half):
    return half + half * jnp.tanh(half)


def layer_kernel(
    maps_hbm, late_hbm, proj_hbm, outw_hbm, first_hbm, mixed_hbm,
    maps_ref, late_ref, proj_ref, outw_ref, first_ref,
    flat, emb, gates, vals, quer, keys, att, mixed_ref, out_sem, in_sem,
):
    seq_len = mixed_hbm.shape[1]
    loads = [
        pltpu.make_async_copy(source, target, in_sem.at[i])
        for i, (source, target) in enumerate(
            (
                (maps_hbm, maps_ref), (late_hbm, late_ref), (proj_hbm, proj_ref),
                (outw_hbm, outw_ref), (first_hbm, first_ref),
            )
        )
    ]
    for load in loads:
        load.start()
    for load in loads[:2]:
        load.wait()
    long_at = jnp.where(maps_ref[0, 0, CAP + 17] > maps_ref[0, 1, CAP + 17], 1, 0)
    move = pltpu.make_async_copy(first_ref, mixed_hbm.at[long_at], in_sem.at[7])

    def weights():
        for load in loads[2:]:
            load.wait()
        move.start()

    def put(b):
        return store_block(b, mixed_ref, mixed_hbm.at[1 - long_at], out_sem)

    layer_history(
        1, False, maps_ref, late_ref, proj_ref, outw_ref, put,
        flat, emb, gates, vals, quer, keys, att, mixed_ref, weights, move.wait,
    )
    for b in range(seq_len // BLOCK):
        put(b).wait()


def store_block(b, mixed_ref, mixed_hbm, out_sem):
    span = pl.ds(b * BLOCK, BLOCK)
    return pltpu.make_async_copy(mixed_ref.at[span], mixed_hbm.at[span], out_sem.at[b])


def layer_history(
    seq, whole, maps_ref, got_ref, proj_ref, outw_ref, put,
    flat, emb, gates, vals, quer, keys, att, mixed_ref, weights=None, ready=None,
):
    seq_len, width = mixed_ref.shape
    head = width // HEADS
    length = maps_ref[0, seq, CAP + 16]
    side = width // 4
    half = got_ref.shape[1]
    shards = got_ref.shape[0] // 4
    group = 8
    first_half = lax.broadcasted_iota(I32, (1, 1, 2 * side), 2) < side

    def place_blocks(c, carry):
        rows = group * 2 * half
        at = pl.multiple_of(c * rows, rows)
        for tile in range(2):
            low, high = (
                got_ref[pl.ds((2 * tile + i) * shards + c * group, group)].astype(F32)
                for i in range(2)
            )
            upper = jnp.where(first_half, low, pltpu.roll(high, side, 2))
            lower = jnp.where(first_half, pltpu.roll(low, side, 2), high)
            flat[tile, pl.ds(at, rows), :] = jnp.concatenate([upper, lower], axis=1).reshape(
                rows, 2 * side
            )
        return carry

    lax.fori_loop(0, shards // group, place_blocks, 0)

    unroll = 16

    def fetch(c, carry):
        for i in range(unroll):
            slot = maps_ref[c, seq, CAP + i]
            for tile in range(2):
                emb[tile, c, pl.ds(i, 1), :] = flat[tile, pl.ds(slot, 1), :]
        return carry

    lax.fori_loop(0, seq_len // unroll if whole else (length + unroll - 1) // unroll, fetch, 0)

    def rows_of(b):
        span = pl.ds(b * (BLOCK // unroll), BLOCK // unroll)
        return jnp.concatenate([emb[t, span].reshape(BLOCK, 2 * side) for t in range(2)], axis=1)

    blocks = seq_len // BLOCK if whole else (length + BLOCK - 1) // BLOCK
    place = lax.broadcasted_iota(I32, (BLOCK, 1), 0)

    def project(b, carry):
        at = pl.multiple_of(b * BLOCK, BLOCK)
        span = pl.ds(at, BLOCK)
        rows = jnp.where(place + at < length, rows_of(b), 0.0)
        normed = normed_rows(rows).astype(BF16)
        for part, ref in enumerate((gates, vals, quer, keys)):
            raw = jnp.dot(
                normed, proj_ref[:, part * width : (part + 1) * width], preferred_element_type=F32
            )
            made = gated_linear(raw * 0.5).astype(BF16)
            if part == 0:
                ref[span, :] = made
            else:
                if part == 2:
                    made = made * (0.5 / math.sqrt(head))
                for h in range(HEADS):
                    ref[h, span, :] = made[:, h * head : (h + 1) * head]
        return carry

    if weights is not None:
        weights()
    lax.fori_loop(0, blocks, project, 0)
    inverse = 1.0 / length.astype(F32)
    if ready is not None:
        ready()
    keep = lax.broadcasted_iota(I32, (BLOCK, BLOCK), 1) <= lax.broadcasted_iota(
        I32, (BLOCK, BLOCK), 0
    )

    def run(b):
        reach = (b + 1) * BLOCK

        def attend(h, carry):
            query = quer[h, b * BLOCK : reach, :]
            scores = lax.dot_general(
                query, keys[h, :reach, :], (((1,), (1,)), ((), ())), preferred_element_type=F32
            )
            weights = gated_linear(scores)
            last = jnp.where(keep, weights[:, b * BLOCK :], 0.0).astype(BF16)
            if b:
                last = jnp.concatenate([weights[:, : b * BLOCK].astype(BF16), last], axis=1)
            att[h] = jnp.dot(last, vals[h, :reach, :], preferred_element_type=F32)
            return carry

        lax.fori_loop(0, HEADS, attend, 0)
        joined = jnp.concatenate([att[h] for h in range(HEADS)], axis=1) * inverse
        gated = (normed_rows(joined) * gates[b * BLOCK : reach, :].astype(F32)).astype(BF16)
        mixed = rows_of(b) + jnp.dot(gated, outw_ref[...], preferred_element_type=F32)
        live = place + b * BLOCK < length
        mixed_ref[b * BLOCK : reach, :] = jnp.where(live, mixed, 0.0).astype(BF16)

    for b in range(seq_len // BLOCK):
        if whole:
            run(b)
        else:
            pl.when(b * BLOCK < length)(lambda b=b: run(b))

            @pl.when(b * BLOCK >= length)
            def _(b=b):
                mixed_ref[b * BLOCK : (b + 1) * BLOCK, :] = jnp.zeros((BLOCK, width), BF16)

        put(b).start()


def layer(maps, late, first, proj_weight, out_weight):
    slots = maps.shape[0] * CAP
    seq_len, width = first.shape
    return pl.pallas_call(
        layer_kernel,
        out_shape=jax.ShapeDtypeStruct((maps.shape[1], seq_len, width), BF16),
        in_specs=[pl.BlockSpec(memory_space=pltpu.HBM)] * 5,
        out_specs=pl.BlockSpec(memory_space=pltpu.HBM),
        scratch_shapes=[
            pltpu.SMEM(maps.shape, I32),
            pltpu.VMEM(late.shape, BF16),
            pltpu.VMEM(proj_weight.shape, BF16),
            pltpu.VMEM(out_weight.shape, BF16),
            pltpu.VMEM(first.shape, BF16),
            *layer_scratch(seq_len, width, slots),
            pltpu.SemaphoreType.DMA((8,)),
        ],
        compiler_params=pltpu.CompilerParams(vmem_limit_bytes=60 * 1024 * 1024),
        name="layer",
    )(maps, late, proj_weight, out_weight, first)


def body(item_ids, seq_lengths, seq_owner, row_home, item_table, proj_weight, out_weight):
    shards = lax.axis_size("shard")
    late, maps, first = exchange_rows(
        item_ids, seq_lengths, seq_owner, row_home, item_table.T, proj_weight, out_weight, shards
    )
    return layer(maps, late, first, proj_weight, out_weight)


def solution(mesh):
    in_specs = (
        P(("rep", "shard"), None),
        P("rep", None),
        P("rep", None),
        P(),
        P("shard", "rep"),
        P(),
        P(),
    )
    out_specs = P(("rep", "shard"), None, None)
    return jax.shard_map(body, mesh=mesh, in_specs=in_specs, out_specs=out_specs, check_vma=False)
```
